8 devices in a mesh: dp: 1 (over z), tp: 2 (over y), sp: 4 (over x, core).
Axes of the slice: x: 2, y: 2, z: 1, core: 2. Of those that a mesh axis runs over, the one named last changes fastest.
Arguments:
- layer_in: bfloat16 [32, 5120], P('dp')
- new_pos: int32 [32], P('dp')
- k_cache: bfloat16 [32, 512, 40, 128], P('dp', 'sp', 'tp')
- v_cache: bfloat16 [32, 512, 40, 128], P('dp', 'sp', 'tp')
- attn_gain: bfloat16 [5120], replicated
- w_query: bfloat16 [5120, 5120], P(None, 'tp')
- w_key: bfloat16 [5120, 5120], P(None, 'tp')
- w_value: bfloat16 [5120, 5120], P(None, 'tp')
- w_out: bfloat16 [5120, 5120], P('tp')
- mlp_gain: bfloat16 [5120], replicated
- w_gate: bfloat16 [5120, 13824], P(None, 'tp')
- w_up: bfloat16 [5120, 13824], P(None, 'tp')
- w_down: bfloat16 [13824, 5120], P('tp')
Outputs:
- output 1: bfloat16 [32, 5120], P('dp')
- output 2: bfloat16 [32, 512, 40, 128], P('dp', 'sp', 'tp')
- output 3: bfloat16 [32, 512, 40, 128], P('dp', 'sp', 'tp')
- output 4: bfloat16 [32, 40, 128], P('dp', 'tp')
- output 5: bfloat16 [32, 40, 128], P('dp', 'tp')
All inputs are finite; a program needn't handle non-finite values.
Results may differ from the reference program's by a relative error of at most 0.00497829.
Values sent between devices are 32-bit elements.
A program may use at most 1.5 GiB of HBM per device.

```python
import jax
import jax.numpy as jnp
from jax import lax

BATCH_ROWS = 32
CACHE_LEN = 512
MODEL_DIM = 5120
NUM_HEADS = 40
KV_HEADS = 40
HEAD_DIM = 128
FFN_DIM = 13824
ROPE_THETA = 1000000
COARSE_GROUPS = 64
GROUP_SIZE = NUM_HEADS // KV_HEADS
SCORE_SCALE = HEAD_DIM ** -0.5
MIN_POS = CACHE_LEN // 16


def weight(key_w, w_shape, fan_in):
    return (jax.random.normal(key_w, w_shape, jnp.float32) * fan_in ** -0.5).astype(jnp.bfloat16)


def setup_inputs(seed: int = 0, part: int = 0) -> dict:
    part_key = jax.random.fold_in(jax.random.key(seed), part)
    row_keys = jax.random.split(part_key, 7)
    w_keys = jax.random.split(jax.random.key(seed + 1), 9)
    layer_in = jax.random.normal(row_keys[0], (BATCH_ROWS, MODEL_DIM), jnp.float32).astype(jnp.bfloat16)
    pos_draw = jax.random.randint(row_keys[1], (BATCH_ROWS,), MIN_POS, CACHE_LEN)
    new_pos = jnp.where(jnp.arange(BATCH_ROWS) == 0, CACHE_LEN - 1, pos_draw).astype(jnp.int32)
    cache_shape = (BATCH_ROWS, CACHE_LEN, KV_HEADS, HEAD_DIM)
    coarse_shape = (BATCH_ROWS, COARSE_GROUPS, 1, KV_HEADS, HEAD_DIM)
    span_shape = (BATCH_ROWS, COARSE_GROUPS, CACHE_LEN // COARSE_GROUPS, KV_HEADS, HEAD_DIM)
    k_coarse = jnp.broadcast_to(jax.random.normal(row_keys[2], coarse_shape, jnp.float32), span_shape).reshape(cache_shape)
    v_coarse = jnp.broadcast_to(jax.random.normal(row_keys[3], coarse_shape, jnp.float32), span_shape).reshape(cache_shape)
    k_cache = (jax.random.normal(row_keys[4], cache_shape, jnp.float32) + 1.5 * k_coarse).astype(jnp.bfloat16)
    v_cache = (0.5 * jax.random.normal(row_keys[5], cache_shape, jnp.float32) + 2.0 * v_coarse).astype(jnp.bfloat16)
    attn_gain = (1.0 + 0.2 * jax.random.normal(w_keys[0], (MODEL_DIM,), jnp.float32)).astype(jnp.bfloat16)
    mlp_gain = (1.0 + 0.2 * jax.random.normal(w_keys[1], (MODEL_DIM,), jnp.float32)).astype(jnp.bfloat16)
    return {
        'layer_in': layer_in,
        'new_pos': new_pos,
        'k_cache': k_cache,
        'v_cache': v_cache,
        'attn_gain': attn_gain,
        'w_query': weight(w_keys[2], (MODEL_DIM, NUM_HEADS * HEAD_DIM), MODEL_DIM),
        'w_key': weight(w_keys[3], (MODEL_DIM, KV_HEADS * HEAD_DIM), MODEL_DIM),
        'w_value': weight(w_keys[4], (MODEL_DIM, KV_HEADS * HEAD_DIM), MODEL_DIM),
        'w_out': weight(w_keys[5], (NUM_HEADS * HEAD_DIM, MODEL_DIM), NUM_HEADS * HEAD_DIM),
        'mlp_gain': mlp_gain,
        'w_gate': weight(w_keys[6], (MODEL_DIM, FFN_DIM), MODEL_DIM),
        'w_up': weight(w_keys[7], (MODEL_DIM, FFN_DIM), MODEL_DIM),
        'w_down': weight(w_keys[8], (FFN_DIM, MODEL_DIM), FFN_DIM),
    }


def rms_norm(in_vec, gain_vec):
    mean_sq = jnp.mean(jnp.square(in_vec), axis=-1, keepdims=True)
    return in_vec * lax.rsqrt(mean_sq + 1e-5) * gain_vec.astype(jnp.float32)


def apply_rotary(in_vec, positions):
    half_idx = jnp.arange(HEAD_DIM // 2, dtype=jnp.float32)
    inv_freq = 1.0 / (ROPE_THETA ** (2.0 * half_idx / HEAD_DIM))
    angles = positions.astype(jnp.float32)[:, None] * inv_freq[None, :]
    cos_a = jnp.cos(angles)[:, None, :]
    sin_a = jnp.sin(angles)[:, None, :]
    pair_view = in_vec.reshape(in_vec.shape[:-1] + (HEAD_DIM // 2, 2))
    even_part = pair_view[..., 0]
    odd_part = pair_view[..., 1]
    rotated = jnp.stack([even_part * cos_a - odd_part * sin_a, even_part * sin_a + odd_part * cos_a], axis=-1)
    return rotated.reshape(in_vec.shape)


def reference(layer_in, new_pos, k_cache, v_cache, attn_gain, w_query, w_key, w_value, w_out, mlp_gain, w_gate, w_up, w_down):
    x_f32 = layer_in.astype(jnp.float32)
    normed = rms_norm(x_f32, attn_gain).astype(jnp.bfloat16)
    q_proj = jnp.dot(normed, w_query, preferred_element_type=jnp.float32).reshape(BATCH_ROWS, NUM_HEADS, HEAD_DIM)
    k_proj = jnp.dot(normed, w_key, preferred_element_type=jnp.float32).reshape(BATCH_ROWS, KV_HEADS, HEAD_DIM)
    v_new = jnp.dot(normed, w_value, preferred_element_type=jnp.float32).reshape(BATCH_ROWS, KV_HEADS, HEAD_DIM).astype(jnp.bfloat16)
    q_rot = apply_rotary(q_proj, new_pos).astype(jnp.bfloat16)
    k_rot = apply_rotary(k_proj, new_pos).astype(jnp.bfloat16)
    slot_ids = jnp.arange(CACHE_LEN)

    def one_row(row_args):
        q_row, k_row, v_row, k_rows, v_rows, pos_row = row_args
        is_new = (slot_ids == pos_row)[:, None, None]
        k_upd = jnp.where(is_new, k_row[None], k_rows)
        v_upd = jnp.where(is_new, v_row[None], v_rows)
        q_grp = q_row.reshape(KV_HEADS, GROUP_SIZE, HEAD_DIM).astype(jnp.float32)
        scores = jnp.einsum('kgd,skd->kgs', q_grp, k_upd.astype(jnp.float32)) * SCORE_SCALE
        scores = jnp.where(slot_ids <= pos_row, scores, -jnp.inf)
        row_max = jnp.max(scores, axis=-1, keepdims=True)
        prob_vals = jnp.exp(scores - row_max)
        denom_sum = jnp.sum(prob_vals, axis=-1)
        weighted = jnp.einsum('kgs,skd->kgd', prob_vals.astype(jnp.bfloat16).astype(jnp.float32), v_upd.astype(jnp.float32))
        attn_row = (weighted / denom_sum[..., None]).reshape(NUM_HEADS * HEAD_DIM)
        return attn_row, k_upd, v_upd

    attn_rows, k_out, v_out = lax.map(one_row, (q_rot, k_rot, v_new, k_cache, v_cache, new_pos))
    attn_vec = attn_rows.astype(jnp.bfloat16)
    hidden = x_f32 + jnp.dot(attn_vec, w_out, preferred_element_type=jnp.float32)
    normed_mlp = rms_norm(hidden, mlp_gain).astype(jnp.bfloat16)
    gate_pre = jnp.dot(normed_mlp, w_gate, preferred_element_type=jnp.float32)
    up_proj = jnp.dot(normed_mlp, w_up, preferred_element_type=jnp.float32)
    act_bf = (jax.nn.silu(gate_pre) * up_proj).astype(jnp.bfloat16)
    layer_out = (hidden + jnp.dot(act_bf, w_down, preferred_element_type=jnp.float32)).astype(jnp.bfloat16)
    return (layer_out, k_out, v_out, k_rot, v_new)
```

```python
import functools

import jax
import jax.numpy as jnp
import numpy as np
from jax import lax
from jax.experimental import pallas as pl
from jax.experimental.pallas import tpu as pltpu
from jax.sharding import PartitionSpec as P

ROPE_THETA = 1000000
MESH = pl.DeviceIdType.MESH
F32 = jnp.float32
BF16 = jnp.bfloat16
NEG = float(np.finfo(np.float32).min)

ROWS = 32
DIM = 5120
HEADS = 20
HD = 128
SLOTS = 128
SHARD = 640
PADH = 24
FFN_SHARD = 1792
FFN_LOC = 6912


def vmem():
    return pl.BlockSpec(memory_space=pltpu.VMEM)


def smem():
    return pl.BlockSpec(memory_space=pltpu.SMEM)


def hbm():
    return pl.BlockSpec(memory_space=pl.ANY)


def remote(src, dst, send_sem, recv_sem, device):
    return pltpu.make_async_remote_copy(src_ref=src, dst_ref=dst, send_sem=send_sem, recv_sem=recv_sem,
                                        device_id=device, device_id_type=MESH)


def enter_barrier(partners):
    barrier = pltpu.get_barrier_semaphore()
    for partner in partners:
        pl.semaphore_signal(barrier, inc=1, device_id=partner, device_id_type=MESH)
    pl.semaphore_wait(barrier, len(partners))


QK_CH = 4


def qkv_kernel(pos_ref, x_ref, gain_ref, freq_ref, wq, wk, wv, q_out, k_out, v_out,
               wq_buf, wk_buf, wv_buf, n_buf, pieces, q_pieces,
               sem_q, sem_k, sem_v, d2d_s, d2d_r, ici_s, ici_r, fwd_s, fwd_r, q_s, q_r):
    s = lax.axis_index("sp")
    c = lax.rem(s, 2)
    xc = s // 2
    core_peer = 2 * xc + (1 - c)
    x_peer = 2 * (1 - xc) + c

    rows = DIM // QK_CH
    col = pl.multiple_of(s * SHARD, SHARD)
    qcol = pl.multiple_of(c * 2 * SHARD, 2 * SHARD)

    def weight_copy(src, buf, sem, i, start, width):
        r = pl.ds(i * rows, rows)
        return pltpu.make_async_copy(src.at[r, pl.ds(start, width)], buf.at[r, :], sem.at[i])

    k_copies = [weight_copy(wk, wk_buf, sem_k, i, col, SHARD) for i in range(QK_CH)]
    v_copies = [weight_copy(wv, wv_buf, sem_v, i, col, SHARD) for i in range(QK_CH)]
    q_copies = [weight_copy(wq, wq_buf, sem_q, i, qcol, 2 * SHARD) for i in range(QK_CH)]
    for cp in k_copies + v_copies + q_copies:
        cp.start()

    x = x_ref[...].astype(F32)
    mean_sq = jnp.mean(jnp.square(x), axis=-1, keepdims=True)
    n_buf[...] = (x * lax.rsqrt(mean_sq + 1e-5) * gain_ref[...].astype(F32)).astype(BF16)

    row_id = lax.broadcasted_iota(jnp.int32, (ROWS, HD), 0)
    lane = lax.broadcasted_iota(jnp.int32, (ROWS, HD), 1)
    pos = jnp.zeros((ROWS, HD), jnp.int32)
    for r in range(ROWS):
        pos = jnp.where(row_id == r, pos_ref[r], pos)
    angle = pos.astype(F32) * freq_ref[...]
    cos_a = jnp.cos(angle)
    even = lax.rem(lane, 2) == 0
    sin_a = jnp.where(even, -jnp.sin(angle), jnp.sin(angle))

    def rope(v):
        swapped = jnp.where(even, pltpu.roll(v, HD - 1, 1), pltpu.roll(v, 1, 1))
        return v * cos_a + swapped * sin_a

    enter_barrier([{"sp": core_peer}, {"sp": x_peer}])

    def project(buf, copies, width):
        acc = jnp.zeros((ROWS, width), F32)
        for i in range(QK_CH):
            copies[i].wait()
            acc += jnp.dot(n_buf[:, i * rows:(i + 1) * rows], buf[i * rows:(i + 1) * rows, :],
                           preferred_element_type=F32)
        return acc

    d2d, ici = [], []
    for m, (buf, copies) in enumerate(((wk_buf, k_copies), (wv_buf, v_copies))):
        acc = project(buf, copies, SHARD)
        for h in range(SHARD // HD):
            part = acc[:, h * HD:(h + 1) * HD]
            pieces[m, s, :, h * HD:(h + 1) * HD] = rope(part) if m == 0 else part
        mine = pieces.at[m, s]
        ici.append(remote(mine, mine, ici_s.at[m], ici_r.at[m], {"sp": x_peer}))
        d2d.append(remote(mine, mine, d2d_s.at[m], d2d_r.at[m], {"sp": core_peer}))
        ici[m].start()
        d2d[m].start()

    acc = project(wq_buf, q_copies, 2 * SHARD)
    for h in range(2 * SHARD // HD):
        q_pieces[c, :, h * HD:(h + 1) * HD] = rope(acc[:, h * HD:(h + 1) * HD])
    q_cp = remote(q_pieces.at[c], q_pieces.at[c], q_s, q_r, {"sp": core_peer})
    q_cp.start()

    fwd = []
    for m in range(2):
        ici[m].wait_recv()
        theirs = pieces.at[m, x_peer]
        fwd.append(remote(theirs, theirs, fwd_s.at[m], fwd_r.at[m], {"sp": core_peer}))
        fwd[m].start()
    q_cp.wait()
    for i in range(2):
        q_out[:, i * 2 * SHARD:(i + 1) * 2 * SHARD] = q_pieces[i]
    for m, out in enumerate((k_out, v_out)):
        d2d[m].wait()
        fwd[m].wait()
        ici[m].wait_send()
        for i in range(4):
            out[:, i * SHARD:(i + 1) * SHARD] = pieces[m, i]


def qkv_call(pos, x, gain, freq, wq, wk, wv):
    out = jax.ShapeDtypeStruct((ROWS, HEADS * HD), F32)
    dma = pltpu.SemaphoreType.DMA
    return pl.pallas_call(
        qkv_kernel,
        out_shape=(out, out, out),
        in_specs=[smem(), vmem(), vmem(), vmem(), hbm(), hbm(), hbm()],
        out_specs=(vmem(), vmem(), vmem()),
        scratch_shapes=[
            pltpu.VMEM((DIM, 2 * SHARD), BF16), pltpu.VMEM((DIM, SHARD), BF16), pltpu.VMEM((DIM, SHARD), BF16),
            pltpu.VMEM((ROWS, DIM), BF16),
            pltpu.VMEM((2, 4, ROWS, SHARD), F32), pltpu.VMEM((2, ROWS, 2 * SHARD), F32),
            dma((QK_CH,)), dma((QK_CH,)), dma((QK_CH,)),
            dma((2,)), dma((2,)), dma((2,)), dma((2,)), dma((2,)), dma((2,)), dma, dma,
        ],
        compiler_params=pltpu.CompilerParams(collective_id=0, has_side_effects=True, vmem_limit_bytes=48 << 20),
        name="qkv",
    )(pos, x, gain, freq, wq, wk, wv)


RING = 8
AHEAD = 4
STEP_ROWS = 2


def attn_kernel(pos_ref, q_ref, k_ref, v_ref, kc, vc, ko, vo, kn_ref, vn_ref, op_ref,
                kbuf, vbuf, q3, k3, v3, o3, st, sem_ki, sem_vi, sem_ko, sem_vo):
    s = lax.axis_index("sp")
    base = s * SLOTS

    def in_copies(b, slot):
        return (pltpu.make_async_copy(kc.at[b], kbuf.at[slot], sem_ki.at[slot]),
                pltpu.make_async_copy(vc.at[b], vbuf.at[slot], sem_vi.at[slot]))

    def out_copies(b, slot):
        return (pltpu.make_async_copy(kbuf.at[slot], ko.at[b], sem_ko.at[slot]),
                pltpu.make_async_copy(vbuf.at[slot], vo.at[b], sem_vo.at[slot]))

    for b in range(AHEAD):
        for cp in in_copies(b, b):
            cp.start()

    for h in range(HEADS):
        sl = slice(h * HD, (h + 1) * HD)
        q3[pl.ds(h, ROWS, stride=PADH), :] = q_ref[:, sl]
        k3[pl.ds(h, ROWS, stride=PADH), :] = k_ref[:, sl]
        v3[pl.ds(h, ROWS, stride=PADH), :] = v_ref[:, sl]
        kn_ref[h] = k_ref[:, sl].astype(BF16)
        vn_ref[h] = v_ref[:, sl].astype(BF16)
    st[...] = jnp.zeros_like(st)

    lane = lax.broadcasted_iota(jnp.int32, (8, HD), 1)
    sub = lax.broadcasted_iota(jnp.int32, (8, HD), 0)
    scale = HD ** -0.5

    def row_attention(b, slot):
        rel = pos_ref[b] - base

        @pl.when(jnp.logical_and(rel >= 0, rel < SLOTS))
        def _():
            start = pl.multiple_of((rel // 16) * 16, 16)
            here = lax.broadcasted_iota(jnp.int32, (16, HD), 0) == rel - start
            for h in range(HEADS):
                for buf, new in ((kbuf, k3), (vbuf, v3)):
                    row = jnp.broadcast_to(new[pl.ds(b * PADH + h, 1), :], (16, HD))
                    old = buf[slot, h, pl.ds(start, 16), :].astype(F32)
                    buf[slot, h, pl.ds(start, 16), :] = jnp.where(here, row, old).astype(BF16)

        valid = lane <= rel
        at_b = lane == b
        for g in range(0, HEADS, 8):
            row0 = pl.multiple_of(b * PADH + g, 8)
            qg = q3[pl.ds(row0, 8), :].astype(BF16)
            n = min(8, HEADS - g)
            sc = jnp.zeros((8, HD), F32)
            for h in range(n):
                one = lax.dot_general(qg, kbuf[slot, g + h], (((1,), (1,)), ((), ())), preferred_element_type=F32)
                sc = jnp.where(sub == h, one, sc)
            sc = jnp.where(valid, sc * scale, NEG)
            top = jnp.max(sc, axis=-1, keepdims=True)
            w = jnp.where(valid, jnp.exp(sc - top), 0.0)
            total = jnp.sum(w, axis=-1, keepdims=True)
            wb = w.astype(BF16)
            acc = jnp.zeros((8, HD), F32)
            for h in range(n):
                one = jnp.dot(wb, vbuf[slot, g + h], preferred_element_type=F32)
                acc = jnp.where(sub == h, one, acc)
            o3[pl.ds(row0, 8), :] = acc
            st[g:g + 8, :] = jnp.where(at_b, top, st[g:g + 8, :])
            st[64 + g:64 + g + 8, :] = jnp.where(at_b, total, st[64 + g:64 + g + 8, :])

    def step(i, carry):
        for j in range(STEP_ROWS):
            b = i * STEP_ROWS + j
            nxt = b + AHEAD
            nslot = lax.rem(nxt, RING)

            @pl.when(nxt < ROWS)
            def _():
                @pl.when(nxt >= RING)
                def _():
                    for cp in out_copies(nxt - RING, nslot):
                        cp.wait()
                for cp in in_copies(nxt, nslot):
                    cp.start()
        for j in range(STEP_ROWS):
            b = i * STEP_ROWS + j
            for cp in in_copies(b, lax.rem(b, RING)):
                cp.wait()
        for j in range(STEP_ROWS):
            b = i * STEP_ROWS + j
            row_attention(b, lax.rem(b, RING))
        for j in range(STEP_ROWS):
            b = i * STEP_ROWS + j
            for cp in out_copies(b, lax.rem(b, RING)):
                cp.start()
        return carry

    lax.fori_loop(0, ROWS // STEP_ROWS, step, 0)

    stats = jnp.transpose(st[...])[:ROWS, :]
    for c in range(2):
        for xc in range(2):
            o = 2 * xc + c
            for j in range(5):
                op_ref[2 * c + xc, j] = o3[pl.ds(5 * o + j, ROWS, stride=PADH), :]
            op_ref[2 * c + xc, 5] = pltpu.roll(stats, HD - 5 * o, 1) if o else stats
    for b in range(ROWS - RING, ROWS):
        for cp in out_copies(b, b % RING):
            cp.wait()


def attn_call(pos, q, k, v, kc, vc):
    cache = jax.ShapeDtypeStruct((ROWS, HEADS, SLOTS, HD), BF16)
    new = jax.ShapeDtypeStruct((HEADS, ROWS, HD), BF16)
    part = jax.ShapeDtypeStruct((4, 6, ROWS, HD), F32)
    dma = pltpu.SemaphoreType.DMA
    flat = pltpu.VMEM((ROWS * PADH, HD), F32)
    return pl.pallas_call(
        attn_kernel,
        out_shape=(cache, cache, new, new, part),
        in_specs=[smem(), vmem(), vmem(), vmem(), hbm(), hbm()],
        out_specs=(hbm(), hbm(), vmem(), vmem(), vmem()),
        scratch_shapes=[
            pltpu.VMEM((RING, HEADS, SLOTS, HD), BF16), pltpu.VMEM((RING, HEADS, SLOTS, HD), BF16),
            flat, flat, flat, flat, pltpu.VMEM((HD, HD), F32),
            dma((RING,)), dma((RING,)), dma((RING,)), dma((RING,)),
        ],
        compiler_params=pltpu.CompilerParams(vmem_limit_bytes=32 << 20),
        name="attn",
    )(pos, q, k, v, kc, vc)


WO_ROWS = 640
D_FIRST = 768
D_REST = FFN_SHARD - D_FIRST
PIECE = 640


def combine(a_o, a_st, b_o, b_st):
    lane = lax.broadcasted_iota(jnp.int32, (ROWS, HD), 1)
    is_max = lane < 64
    top = jnp.maximum(a_st, b_st)
    fa = jnp.exp(jnp.where(is_max, a_st - top, 0.0))
    fb = jnp.exp(jnp.where(is_max, b_st - top, 0.0))
    total = pltpu.roll(fa, 64, 1) * a_st + pltpu.roll(fb, 64, 1) * b_st
    out = [fa[:, j:j + 1] * a_o[j] + fb[:, j:j + 1] * b_o[j] for j in range(5)]
    return out, jnp.where(is_max, top, total)


def mlp_kernel(op_ref, x_ref, gain_ref, wo, wg, wu, wd, out_ref,
               wo_buf, g_buf, u_buf, d_buf, rs1, z, rs2, attn_buf,
               stage_p, r1, stage_h, r2, full1, stage_p2, r1b, stage_h2, r2b, full2, n_buf, a_buf,
               sem_w, rs_s, rs_r, p_s, p_r, h_s, h_r, f_s, f_r, g_s, g_r,
               p_s2, p_r2, h_s2, h_r2, f_s2, f_r2, g_s2, g_r2):
    s = lax.axis_index("sp")
    t = lax.axis_index("tp")
    c = lax.rem(s, 2)
    xc = s // 2
    ot, ox, oc = 1 - t, 1 - xc, 1 - c
    core_dev = {"tp": t, "sp": 2 * xc + oc}
    chips = [(t, xc), (t, ox), (ot, xc), (ot, ox)]
    devs = [{"tp": ct, "sp": 2 * cx + c} for ct, cx in chips]
    chip_id = [2 * ct + cx for ct, cx in chips]

    wo_row = pl.multiple_of(s * WO_ROWS, WO_ROWS)
    start = pl.multiple_of(jnp.minimum(s * FFN_SHARD, FFN_LOC - FFN_SHARD), 256)
    cols = pl.ds(start, FFN_SHARD)
    half = DIM // 2

    wo_cp = pltpu.make_async_copy(wo.at[pl.ds(wo_row, WO_ROWS), :], wo_buf.at[pl.ds(0, WO_ROWS), :], sem_w.at[0])
    g_cps = [pltpu.make_async_copy(wg.at[pl.ds(i * half, half), cols], g_buf.at[pl.ds(i * half, half), :],
                                   sem_w.at[1 + i]) for i in range(2)]
    u_cps = [pltpu.make_async_copy(wu.at[pl.ds(i * half, half), cols], u_buf.at[pl.ds(i * half, half), :],
                                   sem_w.at[3 + i]) for i in range(2)]
    d_cp = pltpu.make_async_copy(wd.at[pl.ds(start + D_FIRST, D_REST), :], d_buf, sem_w.at[5])
    d0_cp = pltpu.make_async_copy(wd.at[pl.ds(start, D_FIRST), :], wo_buf, sem_w.at[6])
    for cp in [wo_cp] + g_cps + u_cps + [d_cp]:
        cp.start()

    enter_barrier([core_dev] + devs[1:])

    first = remote(op_ref.at[pl.ds(oc * 2, 2)], rs1, rs_s.at[0], rs_r.at[0], core_dev)
    first.start()
    first.wait_recv()

    def merge(i):
        mine = 2 * c + i
        return combine([op_ref[mine, j] for j in range(5)], op_ref[mine, 5],
                       [rs1[i, j] for j in range(5)], rs1[i, 5])

    o_out, st_out = merge(ox)
    for j in range(5):
        z[j] = o_out[j]
    z[5] = st_out
    second = remote(z, rs2, rs_s.at[1], rs_r.at[1], devs[1])
    second.start()
    o_own, st_own = merge(xc)
    second.wait_recv()
    o_all, st_all = combine(o_own, st_own, [rs2[j] for j in range(5)], rs2[5])
    for j in range(5):
        attn_buf[:, j * HD:(j + 1) * HD] = (o_all[j] / st_all[:, 64 + j:65 + j]).astype(BF16)

    def all_reduce(compute, finish, stage_p, r1, stage_h, r2, full, p_s, p_r, h_s, h_r, f_s, f_r, g_s, g_r):
        order = (3, 1, 2, 0)
        to_core = {}
        for d in order:
            stage_p[d] = compute(oc * 4 + chip_id[d])
            to_core[d] = remote(stage_p.at[d], r1.at[d], p_s.at[d], p_r.at[d], core_dev)
            to_core[d].start()
        to_chip = {}
        own = None
        for d in order:
            part = compute(c * 4 + chip_id[d])
            to_core[d].wait_recv()
            part = part + r1[d]
            if d:
                stage_h[d - 1] = part
                to_chip[d] = remote(stage_h.at[d - 1], r2.at[d - 1], h_s.at[d - 1], h_r.at[d - 1], devs[d])
                to_chip[d].start()
            else:
                own = part
        for d in (1, 2, 3):
            to_chip[d].wait_recv()
            own = own + r2[d - 1]
        mine = c * 4 + chip_id[0]
        full[mine] = finish(own, mine)
        sends = []
        for d in (3, 1, 2):
            cp = remote(full.at[mine], full.at[mine], f_s.at[d - 1], f_r.at[d - 1], devs[d])
            cp.start()
            sends.append((d, cp))
        forward = [remote(full.at[mine], full.at[mine], g_s.at[0], g_r.at[0], core_dev)]
        forward[0].start()
        for d in (1, 2, 3):
            dict(sends)[d].wait_recv()
            piece = full.at[c * 4 + chip_id[d]]
            cp = remote(piece, piece, g_s.at[d], g_r.at[d], core_dev)
            cp.start()
            forward.append(cp)
        for cp in forward:
            cp.wait_recv()
        for cp in forward + [cp for _, cp in sends] + [to_chip[d] for d in (1, 2, 3)] + [to_core[d] for d in order]:
            cp.wait_send()

    def piece_cols(i):
        return pl.ds(pl.multiple_of(i * PIECE, PIECE), PIECE)

    wo_cp.wait()
    all_reduce(lambda i: jnp.dot(attn_buf[...], wo_buf[:WO_ROWS, piece_cols(i)], preferred_element_type=F32),
               lambda v, i: v + x_ref[:, piece_cols(i)].astype(F32),
               stage_p, r1, stage_h, r2, full1, p_s, p_r, h_s, h_r, f_s, f_r, g_s, g_r)
    first.wait_send()
    second.wait_send()
    d0_cp.start()

    sq = jnp.zeros((ROWS, 1), F32)
    for i in range(8):
        sq += jnp.sum(jnp.square(full1[i]), axis=-1, keepdims=True)
    inv = lax.rsqrt(sq / DIM + 1e-5)
    for i in range(8):
        sl = slice(i * PIECE, (i + 1) * PIECE)
        n_buf[:, sl] = (full1[i] * inv * gain_ref[:, sl].astype(F32)).astype(BF16)

    for cp in g_cps + u_cps:
        cp.wait()
    skip = s * FFN_SHARD - start

    def hidden(j, carry):
        at = pl.ds(pl.multiple_of(j * 256, 256), 256)
        gate = jnp.dot(n_buf[...], g_buf[:, at], preferred_element_type=F32)
        up = jnp.dot(n_buf[...], u_buf[:, at], preferred_element_type=F32)
        act = gate / (1.0 + jnp.exp(-gate)) * up
        col = lax.broadcasted_iota(jnp.int32, (ROWS, 256), 1) + j * 256
        a_buf[:, at] = jnp.where(col >= skip, act, 0.0).astype(BF16)
        return carry

    lax.fori_loop(0, FFN_SHARD // 256, hidden, 0)

    d_cp.wait()
    d0_cp.wait()

    def down(i):
        at = piece_cols(i)
        return (jnp.dot(a_buf[:, :D_FIRST], wo_buf[:, at], preferred_element_type=F32)
                + jnp.dot(a_buf[:, D_FIRST:], d_buf[:, at], preferred_element_type=F32))

    all_reduce(down, lambda v, i: v + full1[i],
               stage_p2, r1b, stage_h2, r2b, full2, p_s2, p_r2, h_s2, h_r2, f_s2, f_r2, g_s2, g_r2)
    for i in range(8):
        out_ref[:, i * PIECE:(i + 1) * PIECE] = full2[i].astype(BF16)


def mlp_call(op, x, gain, wo, wg, wu, wd):
    dma = pltpu.SemaphoreType.DMA

    def pieces(n):
        return pltpu.VMEM((n, ROWS, PIECE), F32)

    ar_bufs = [pieces(4), pieces(4), pieces(3), pieces(3), pieces(8)]
    ar_sems = [dma((4,)), dma((4,)), dma((3,)), dma((3,)), dma((3,)), dma((3,)), dma((4,)), dma((4,))]
    return pl.pallas_call(
        mlp_kernel,
        out_shape=jax.ShapeDtypeStruct((ROWS, DIM), BF16),
        in_specs=[vmem(), vmem(), vmem(), hbm(), hbm(), hbm(), hbm()],
        out_specs=vmem(),
        scratch_shapes=[
            pltpu.VMEM((D_FIRST, DIM), BF16), pltpu.VMEM((DIM, FFN_SHARD), BF16),
            pltpu.VMEM((DIM, FFN_SHARD), BF16), pltpu.VMEM((D_REST, DIM), BF16),
            pltpu.VMEM((2, 6, ROWS, HD), F32), pltpu.VMEM((6, ROWS, HD), F32), pltpu.VMEM((6, ROWS, HD), F32),
            pltpu.VMEM((ROWS, WO_ROWS), BF16),
        ] + ar_bufs + ar_bufs + [
            pltpu.VMEM((ROWS, DIM), BF16), pltpu.VMEM((ROWS, FFN_SHARD), BF16),
            dma((7,)), dma((2,)), dma((2,)),
        ] + ar_sems + ar_sems,
        compiler_params=pltpu.CompilerParams(collective_id=1, has_side_effects=True, vmem_limit_bytes=62 << 20),
        name="mlp",
    )(op, x, gain, wo, wg, wu, wd)


def solution(mesh):
    half_idx = np.arange(HD // 2, dtype=np.float64)
    freq = np.repeat(1.0 / (ROPE_THETA ** (2.0 * half_idx / HD)), 2).astype(np.float32)[None, :]

    def local_step(layer_in, new_pos, k_blk, v_blk, attn_gain, w_query, w_key, w_value, w_out, mlp_gain, w_gate, w_up, w_down):
        q, k, v = qkv_call(new_pos, layer_in, attn_gain.reshape(1, DIM), jnp.asarray(freq), w_query, w_key, w_value)
        kc = jnp.transpose(k_blk, (0, 2, 1, 3))
        vc = jnp.transpose(v_blk, (0, 2, 1, 3))
        ko, vo, kn, vn, op = attn_call(new_pos, q, k, v, kc, vc)
        out = mlp_call(op, layer_in, mlp_gain.reshape(1, DIM), w_out, w_gate, w_up, w_down)
        back = lambda a: jnp.transpose(a, (0, 2, 1, 3))
        return out, back(ko), back(vo), jnp.transpose(kn, (1, 0, 2)), jnp.transpose(vn, (1, 0, 2))

    cache_spec = P('dp', 'sp', 'tp', None)
    new_spec = P('dp', 'tp', None)
    in_specs = (P('dp', None), P('dp'), cache_spec, cache_spec, P(None), P(None, 'tp'), P(None, 'tp'), P(None, 'tp'), P('tp', None), P(None), P(None, 'tp'), P(None, 'tp'), P('tp', None))
    out_specs = (P('dp', None), cache_spec, cache_spec, new_spec, new_spec)
    return jax.shard_map(local_step, mesh=mesh, in_specs=in_specs, out_specs=out_specs, check_vma=False)
```

```python
import functools

import jax
import jax.numpy as jnp
import numpy as np
from jax import lax
from jax.experimental import pallas as pl
from jax.experimental.pallas import tpu as pltpu
from jax.sharding import PartitionSpec as P

ROPE_THETA = 1000000
MESH = pl.DeviceIdType.MESH
F32 = jnp.float32
BF16 = jnp.bfloat16
NEG = float(np.finfo(np.float32).min)

ROWS = 32
DIM = 5120
HEADS = 20
HD = 128
SLOTS = 128
SHARD = 640
PADH = 24
FFN_SHARD = 1792
FFN_LOC = 6912
HELD = 1536


def vmem():
    return pl.BlockSpec(memory_space=pltpu.VMEM)


def smem():
    return pl.BlockSpec(memory_space=pltpu.SMEM)


def hbm():
    return pl.BlockSpec(memory_space=pltpu.HBM)


def remote(src, dst, send_sem, recv_sem, device):
    return pltpu.make_async_remote_copy(src_ref=src, dst_ref=dst, send_sem=send_sem, recv_sem=recv_sem,
                                        device_id=device, device_id_type=MESH)


def enter_barrier(partners):
    barrier = pltpu.get_barrier_semaphore()
    for partner in partners:
        pl.semaphore_signal(barrier, inc=1, device_id=partner, device_id_type=MESH)
    pl.semaphore_wait(barrier, len(partners))


def scaled_norm(block, inv, gain_ref, n_buf):
    gain = gain_ref[...].astype(F32)
    for i in range(DIM // HD):
        n_buf[:, i * HD:(i + 1) * HD] = (block(i) * inv * gain[i:i + 1, :]).astype(BF16)


QK_CH = 4
Q_CH = 8
KC_ROWS = 2
WINDOW = 4


def qkv_kernel(pos_hbm, x_hbm, gain_hbm, freq_hbm, wq, wk, wv, kc, q_out, k_out, v_out, kc_out,
               pos_ref, x_ref, gain_ref, freq_ref, wq_buf, wk_buf, wv_buf, n_buf, pieces, q_pieces,
               sem_in, sem_kc, sem_q, sem_k, sem_v, d2d_s, d2d_r, ici_s, ici_r, fwd_s, fwd_r, q_s, q_r):
    s = lax.axis_index("sp")
    c = lax.rem(s, 2)
    xc = s // 2
    core_peer = 2 * xc + (1 - c)
    x_peer = 2 * (1 - xc) + c

    col = pl.multiple_of(s * SHARD, SHARD)
    qcol = pl.multiple_of(c * 2 * SHARD, 2 * SHARD)

    def weight_copy(src, buf, sem, i, start, width):
        rows = DIM // (QK_CH if width == SHARD else Q_CH)
        r = pl.ds(i * rows, rows)
        return pltpu.make_async_copy(src.at[r, pl.ds(start, width)], buf.at[r, :], sem.at[i])

    k_copies = [weight_copy(wk, wk_buf, sem_k, i, col, SHARD) for i in range(QK_CH)]
    v_copies = [weight_copy(wv, wv_buf, sem_v, i, col, SHARD) for i in range(QK_CH)]
    q_copies = [weight_copy(wq, wq_buf, sem_q, i, qcol, 2 * SHARD) for i in range(Q_CH)]
    small = [pltpu.make_async_copy(a, b, sem_in.at[i]) for i, (a, b) in enumerate(
        ((x_hbm, x_ref), (gain_hbm, gain_ref), (pos_hbm, pos_ref), (freq_hbm, freq_ref)))]
    cache = [pltpu.make_async_copy(kc.at[pl.ds(i * KC_ROWS, KC_ROWS)], kc_out.at[pl.ds(i * KC_ROWS, KC_ROWS)],
                                   sem_kc.at[i]) for i in range(ROWS // KC_ROWS)]
    stream = k_copies + v_copies + q_copies + cache
    for cp in small + stream[:WINDOW]:
        cp.start()
    pending = stream[WINDOW:]
    for cp in small:
        cp.wait()

    x = x_ref[...].astype(F32)
    mean_sq = jnp.mean(jnp.square(x), axis=-1, keepdims=True)
    scaled_norm(lambda i: x_ref[:, i * HD:(i + 1) * HD].astype(F32), lax.rsqrt(mean_sq + 1e-5), gain_ref, n_buf)

    row_id = lax.broadcasted_iota(jnp.int32, (ROWS, HD), 0)
    lane = lax.broadcasted_iota(jnp.int32, (ROWS, HD), 1)
    pos = jnp.zeros((ROWS, HD), jnp.int32)
    for r in range(ROWS):
        pos = jnp.where(row_id == r, pos_ref[r], pos)
    angle = pos.astype(F32) * freq_ref[...]
    cos_a = jnp.cos(angle)
    even = lax.rem(lane, 2) == 0
    sin_a = jnp.where(even, -jnp.sin(angle), jnp.sin(angle))

    def rope(v):
        swapped = jnp.where(even, pltpu.roll(v, HD - 1, 1), pltpu.roll(v, 1, 1))
        return v * cos_a + swapped * sin_a

    enter_barrier([{"sp": core_peer}, {"sp": x_peer}])

    def project(buf, copies, width):
        acc = jnp.zeros((ROWS, width), F32)
        rows = DIM // len(copies)
        for i in range(len(copies)):
            copies[i].wait()
            if pending:
                pending.pop(0).start()
            acc += jnp.dot(n_buf[:, i * rows:(i + 1) * rows], buf[i * rows:(i + 1) * rows, :],
                           preferred_element_type=F32)
        return acc

    d2d, ici = [], []
    for m, (buf, copies) in enumerate(((wk_buf, k_copies), (wv_buf, v_copies))):
        acc = project(buf, copies, SHARD)
        for h in range(SHARD // HD):
            part = acc[:, h * HD:(h + 1) * HD]
            pieces[m, s, :, h * HD:(h + 1) * HD] = rope(part) if m == 0 else part
        mine = pieces.at[m, s]
        ici.append(remote(mine, mine, ici_s.at[m], ici_r.at[m], {"sp": x_peer}))
        d2d.append(remote(mine, mine, d2d_s.at[m], d2d_r.at[m], {"sp": core_peer}))
        ici[m].start()
        d2d[m].start()

    acc = project(wq_buf, q_copies, 2 * SHARD)
    for cp in pending:
        cp.start()
    for h in range(2 * SHARD // HD):
        q_pieces[c, :, h * HD:(h + 1) * HD] = rope(acc[:, h * HD:(h + 1) * HD])
    q_cp = remote(q_pieces.at[c], q_pieces.at[c], q_s, q_r, {"sp": core_peer})
    q_cp.start()

    fwd = []
    for m in range(2):
        ici[m].wait_recv()
        theirs = pieces.at[m, x_peer]
        fwd.append(remote(theirs, theirs, fwd_s.at[m], fwd_r.at[m], {"sp": core_peer}))
        fwd[m].start()
    q_cp.wait()
    for i in range(2):
        q_out[:, i * 2 * SHARD:(i + 1) * 2 * SHARD] = q_pieces[i]
    for m, out in enumerate((k_out, v_out)):
        d2d[m].wait()
        fwd[m].wait()
        ici[m].wait_send()
        for i in range(4):
            out[:, i * SHARD:(i + 1) * SHARD] = pieces[m, i]
    for cp in cache:
        cp.wait()


def qkv_call(pos, x, gain, freq, wq, wk, wv, kc):
    out = jax.ShapeDtypeStruct((ROWS, HEADS * HD), F32)
    dma = pltpu.SemaphoreType.DMA
    return pl.pallas_call(
        qkv_kernel,
        out_shape=(out, out, out, jax.ShapeDtypeStruct(kc.shape, kc.dtype)),
        in_specs=[hbm()] * 8,
        out_specs=(vmem(), vmem(), vmem(), vmem()),
        scratch_shapes=[
            pltpu.SMEM((ROWS,), jnp.int32), pltpu.VMEM((ROWS, DIM), BF16), pltpu.VMEM((DIM // HD, HD), BF16),
            pltpu.VMEM((1, HD), F32),
            pltpu.VMEM((DIM, 2 * SHARD), BF16), pltpu.VMEM((DIM, SHARD), BF16), pltpu.VMEM((DIM, SHARD), BF16),
            pltpu.VMEM((ROWS, DIM), BF16),
            pltpu.VMEM((2, 4, ROWS, SHARD), F32), pltpu.VMEM((2, ROWS, 2 * SHARD), F32),
            dma((4,)), dma((ROWS // KC_ROWS,)), dma((Q_CH,)), dma((QK_CH,)), dma((QK_CH,)),
            dma((2,)), dma((2,)), dma((2,)), dma((2,)), dma((2,)), dma((2,)), dma, dma,
        ],
        compiler_params=pltpu.CompilerParams(collective_id=0, has_side_effects=True, vmem_limit_bytes=32 << 20),
        name="qkv",
    )(pos, x, gain, freq, wq, wk, wv, kc)


RING = 16
AHEAD = 8
STEP_ROWS = 4


def attn_kernel(pos_ref, q_ref, k_ref, v_ref, kin, vc, ko, vo, kn_ref, vn_ref, op_ref, kbuf,
                vbuf, q3, k3, v3, o3, w3, st, sem_vi, sem_ko, sem_vo):
    s = lax.axis_index("sp")
    base = s * SLOTS

    def v_in(b, slot):
        return pltpu.make_async_copy(vc.at[b], vbuf.at[slot], sem_vi.at[slot])

    def v_out(b, slot):
        return pltpu.make_async_copy(vbuf.at[slot], vo.at[b], sem_vo.at[slot])

    def k_out(b):
        return pltpu.make_async_copy(kbuf.at[b], ko.at[b], sem_ko.at[b])

    for b in range(AHEAD):
        v_in(b, b).start()

    for h in range(HEADS):
        sl = slice(h * HD, (h + 1) * HD)
        q3[pl.ds(h, ROWS, stride=PADH), :] = q_ref[:, sl]
        k3[pl.ds(h, ROWS, stride=PADH), :] = k_ref[:, sl]
        v3[pl.ds(h, ROWS, stride=PADH), :] = v_ref[:, sl]
        kn_ref[h] = k_ref[:, sl].astype(BF16)
        vn_ref[h] = v_ref[:, sl].astype(BF16)
    st[...] = jnp.zeros_like(st)

    lane = lax.broadcasted_iota(jnp.int32, (8, HD), 1)
    sub = lax.broadcasted_iota(jnp.int32, (8, HD), 0)
    even = lax.rem(sub, 2) == 0
    scale = HD ** -0.5

    def patch(b, buf, at, new):
        rel = pos_ref[b] - base

        @pl.when(jnp.logical_and(rel >= 0, rel < SLOTS))
        def _():
            start = pl.multiple_of((rel // 16) * 16, 16)
            here = lax.broadcasted_iota(jnp.int32, (16, HD), 0) == rel - start
            for h in range(HEADS):
                row = jnp.broadcast_to(new[pl.ds(b * PADH + h, 1), :], (16, HD))
                old = buf[at, h, pl.ds(start, 16), :].astype(F32)
                buf[at, h, pl.ds(start, 16), :] = jnp.where(here, row, old).astype(BF16)

    def pair_rows(v):
        return jnp.concatenate([jnp.where(even, v, 0.0), jnp.where(even, 0.0, v)], axis=1).astype(BF16)

    def pick(parts):
        out = parts[-1][:, HD:]
        for i in range(len(parts) - 1, -1, -1):
            if i < len(parts) - 1:
                out = jnp.where(sub < 4 * i + 4, parts[i][:, HD:], out)
            out = jnp.where(sub < 4 * i + 2, parts[i][:, :HD], out)
        return out

    def scores(b, j):
        rel = pos_ref[b] - base
        valid = lane <= rel
        at_b = lane == b
        for g in range(0, HEADS, 8):
            row0 = pl.multiple_of(b * PADH + g, 8)
            qg = pair_rows(q3[pl.ds(row0, 8), :])
            parts = []
            for i in range(min(8, HEADS - g) // 4):
                h = g + 4 * i
                tile = jnp.concatenate([
                    jnp.concatenate([kbuf[b, h], kbuf[b, h + 1]], axis=1),
                    jnp.concatenate([kbuf[b, h + 2], kbuf[b, h + 3]], axis=1)], axis=0)
                parts.append(lax.dot_general(qg, tile, (((1,), (1,)), ((), ())), preferred_element_type=F32))
            sc = jnp.where(valid, pick(parts) * scale, NEG)
            top = jnp.max(sc, axis=-1, keepdims=True)
            w = jnp.where(valid, jnp.exp(sc - top), 0.0)
            total = jnp.sum(w, axis=-1, keepdims=True)
            w3[j * PADH + g:j * PADH + g + 8, :] = w
            st[g:g + 8, :] = jnp.where(at_b, top, st[g:g + 8, :])
            st[64 + g:64 + g + 8, :] = jnp.where(at_b, total, st[64 + g:64 + g + 8, :])

    def values(b, j, slot):
        for g in range(0, HEADS, 8):
            wg = pair_rows(w3[j * PADH + g:j * PADH + g + 8, :])
            parts = []
            for i in range(min(8, HEADS - g) // 4):
                h = g + 4 * i
                tile = jnp.concatenate([
                    jnp.concatenate([vbuf[slot, h], vbuf[slot, h + 2]], axis=1),
                    jnp.concatenate([vbuf[slot, h + 1], vbuf[slot, h + 3]], axis=1)], axis=0)
                parts.append(jnp.dot(wg, tile, preferred_element_type=F32))
            o3[pl.ds(pl.multiple_of(b * PADH + g, 8), 8), :] = pick(parts)

    def step(i, carry):
        rows = [i * STEP_ROWS + j for j in range(STEP_ROWS)]
        for b in rows:
            nxt = b + AHEAD
            nslot = lax.rem(nxt, RING)

            @pl.when(nxt < ROWS)
            def _():
                @pl.when(nxt >= RING)
                def _():
                    v_out(nxt - RING, nslot).wait()
                v_in(nxt, nslot).start()
        for b in rows:
            v_in(b, lax.rem(b, RING)).wait()
        for b in rows:
            patch(b, vbuf, lax.rem(b, RING), v3)
        for b in rows:
            k_out(b).start()
        for j, b in enumerate(rows):
            scores(b, j)

        @pl.when(pos_ref[0] >= 0)
        def _():
            for j, b in enumerate(rows):
                values(b, j, lax.rem(b, RING))

        for b in rows:
            v_out(b, lax.rem(b, RING)).start()

            @pl.when(b + STEP_ROWS < ROWS)
            def _():
                patch(b + STEP_ROWS, kbuf, b + STEP_ROWS, k3)
        return carry

    for b in range(STEP_ROWS):
        patch(b, kbuf, b, k3)
    lax.fori_loop(0, ROWS // STEP_ROWS, step, 0)

    stats = jnp.transpose(st[...])[:ROWS, :]
    for c in range(2):
        for xc in range(2):
            o = 2 * xc + c
            for j in range(5):
                op_ref[2 * c + xc, j] = o3[pl.ds(5 * o + j, ROWS, stride=PADH), :]
            op_ref[2 * c + xc, 5] = pltpu.roll(stats, HD - 5 * o, 1) if o else stats
    for b in range(ROWS - RING, ROWS):
        v_out(b, b % RING).wait()

    def drain(b, carry):
        k_out(b).wait()
        return carry

    lax.fori_loop(0, ROWS, drain, 0)


def attn_call(pos, q, k, v, kc, vc):
    cache = jax.ShapeDtypeStruct((ROWS, HEADS, SLOTS, HD), BF16)
    new = jax.ShapeDtypeStruct((HEADS, ROWS, HD), BF16)
    part = jax.ShapeDtypeStruct((4, 6, ROWS, HD), F32)
    dma = pltpu.SemaphoreType.DMA
    flat = pltpu.VMEM((ROWS * PADH, HD), F32)
    return pl.pallas_call(
        attn_kernel,
        out_shape=(cache, cache, new, new, part, cache),
        in_specs=[smem(), vmem(), vmem(), vmem(), vmem(), hbm()],
        out_specs=(hbm(), hbm(), vmem(), vmem(), vmem(), vmem()),
        input_output_aliases={4: 5},
        scratch_shapes=[
            pltpu.VMEM((RING, HEADS, SLOTS, HD), BF16),
            flat, flat, flat, flat, pltpu.VMEM((STEP_ROWS * PADH, HD), F32), pltpu.VMEM((HD, HD), F32),
            dma((RING,)), dma((ROWS,)), dma((RING,)),
        ],
        compiler_params=pltpu.CompilerParams(vmem_limit_bytes=20 << 20),
        name="attn",
    )(pos, q, k, v, kc, vc)


WO_ROWS = 640
D_FIRST = 768
D_REST = FFN_SHARD - D_FIRST
PIECE = 640
BAND = 16
N_BAND = ROWS // BAND


def combine(a_o, a_st, b_o, b_st):
    lane = lax.broadcasted_iota(jnp.int32, (ROWS, HD), 1)
    is_max = lane < 64
    top = jnp.maximum(a_st, b_st)
    fa = jnp.exp(jnp.where(is_max, a_st - top, 0.0))
    fb = jnp.exp(jnp.where(is_max, b_st - top, 0.0))
    total = pltpu.roll(fa, 64, 1) * a_st + pltpu.roll(fb, 64, 1) * b_st
    out = [fa[:, j:j + 1] * a_o[j] + fb[:, j:j + 1] * b_o[j] for j in range(5)]
    return out, jnp.where(is_max, top, total)


def mlp_kernel(op_ref, x, gain, wo, wg, wu, wd, out_ref,
               wo_buf, g_buf, u_buf, d_buf, rs1, z, rs2, attn_buf,
               stage_p, r1, stage_h, r2, full1, n_buf, a_buf, x_ref, gain_ref,
               sem_w, rs_s, rs_r, p_s, p_r, h_s, h_r, f_s, f_r, g_s, g_r,
               p_s2, p_r2, h_s2, h_r2, f_s2, f_r2, g_s2, g_r2):
    s = lax.axis_index("sp")
    t = lax.axis_index("tp")
    c = lax.rem(s, 2)
    xc = s // 2
    ot, ox, oc = 1 - t, 1 - xc, 1 - c
    core_dev = {"tp": t, "sp": 2 * xc + oc}
    chips = [(t, xc), (t, ox), (ot, xc), (ot, ox)]
    devs = [{"tp": ct, "sp": 2 * cx + c} for ct, cx in chips]
    chip_id = [2 * ct + cx for ct, cx in chips]

    wo_row = pl.multiple_of(s * WO_ROWS, WO_ROWS)
    start = pl.multiple_of(jnp.minimum(s * FFN_SHARD, FFN_LOC - FFN_SHARD), 256)
    half = DIM // 2
    held = pl.ds(start, HELD)
    last = pl.ds(start + HELD, FFN_SHARD - HELD)

    wo_cp = pltpu.make_async_copy(wo.at[pl.ds(wo_row, WO_ROWS), :], wo_buf.at[pl.ds(0, WO_ROWS), :], sem_w.at[0])
    g_cps = [pltpu.make_async_copy(wg.at[pl.ds(i * half, half), held], g_buf.at[pl.ds(i * half, half), :],
                                   sem_w.at[1 + i]) for i in range(2)]
    u_cps = [pltpu.make_async_copy(wu.at[pl.ds(i * half, half), held], u_buf.at[pl.ds(i * half, half), :],
                                   sem_w.at[3 + i]) for i in range(2)]
    d_cp = pltpu.make_async_copy(wd.at[pl.ds(start + D_FIRST, D_REST), :], d_buf, sem_w.at[5])
    d0_cp = pltpu.make_async_copy(wd.at[pl.ds(start, D_FIRST), :], wo_buf, sem_w.at[6])
    own_piece = pl.ds(pl.multiple_of((c * 4 + chip_id[0]) * PIECE, PIECE), PIECE)
    x_cp = pltpu.make_async_copy(x.at[:, own_piece], x_ref, sem_w.at[7])
    gain_cp = pltpu.make_async_copy(gain, gain_ref, sem_w.at[8])
    for cp in (x_cp, gain_cp, wo_cp, g_cps[0]):
        cp.start()
    enter_barrier([core_dev] + devs[1:])

    first = remote(op_ref.at[pl.ds(oc * 2, 2)], rs1, rs_s.at[0], rs_r.at[0], core_dev)
    first.start()
    first.wait_recv()

    def merge(i):
        mine = 2 * c + i
        return combine([op_ref[mine, j] for j in range(5)], op_ref[mine, 5],
                       [rs1[i, j] for j in range(5)], rs1[i, 5])

    o_out, st_out = merge(ox)
    for j in range(5):
        z[j] = o_out[j]
    z[5] = st_out
    second = remote(z, rs2, rs_s.at[1], rs_r.at[1], devs[1])
    second.start()
    o_own, st_own = merge(xc)
    for cp in (x_cp, gain_cp, wo_cp):
        cp.wait()
    for cp in (g_cps[1], u_cps[0], u_cps[1]):
        cp.start()
    second.wait_recv()
    o_all, st_all = combine(o_own, st_own, [rs2[j] for j in range(5)], rs2[5])
    for j in range(5):
        attn_buf[:, j * HD:(j + 1) * HD] = (o_all[j] / st_all[:, 64 + j:65 + j]).astype(BF16)

    def all_reduce(compute, finish, stage_p, r1, stage_h, r2, full, p_s, p_r, h_s, h_r, f_s, f_r, g_s, g_r):
        order = (3, 1, 2, 0)
        bands = [pl.ds(i * BAND, BAND) for i in range(N_BAND)]
        to_core = {}
        for d in order:
            stage_p[d] = compute(oc * 4 + chip_id[d])
            to_core[d] = remote(stage_p.at[d], r1.at[d], p_s.at[d], p_r.at[d], core_dev)
            to_core[d].start()
        own, to_chip = None, {}
        for d in order:
            part = compute(c * 4 + chip_id[d])
            to_core[d].wait_recv()
            part = part + r1[d]
            if d:
                stage_h[d - 1] = part
                for i, band in enumerate(bands):
                    to_chip[d, i] = remote(stage_h.at[d - 1, band], r2.at[d - 1, band], h_s.at[d - 1, i],
                                           h_r.at[d - 1, i], devs[d])
                    to_chip[d, i].start()
            else:
                own = part
        mine = c * 4 + chip_id[0]
        sends, forward = {}, {}
        for i, band in enumerate(bands):
            total = own[i * BAND:(i + 1) * BAND]
            for d in (1, 2, 3):
                to_chip[d, i].wait_recv()
                total = total + r2[d - 1, band]
            full[mine, band] = finish(total, mine, band)
            here = full.at[mine, band]
            for d in (3, 1, 2):
                sends[d, i] = remote(here, here, f_s.at[d - 1, i], f_r.at[d - 1, i], devs[d])
                sends[d, i].start()
            forward[0, i] = remote(here, here, g_s.at[0, i], g_r.at[0, i], core_dev)
            forward[0, i].start()
        for i, band in enumerate(bands):
            for d in (1, 2, 3):
                sends[d, i].wait_recv()
                piece = full.at[c * 4 + chip_id[d], band]
                forward[d, i] = remote(piece, piece, g_s.at[d, i], g_r.at[d, i], core_dev)
                forward[d, i].start()
        for cp in forward.values():
            cp.wait_recv()
        for group in (forward, sends, to_chip, to_core):
            for cp in group.values():
                cp.wait_send()

    def piece_cols(i):
        return pl.ds(pl.multiple_of(i * PIECE, PIECE), PIECE)

    d_cp.start()
    x_f32 = x_ref[...].astype(F32)
    all_reduce(lambda i: jnp.dot(attn_buf[...], wo_buf[:WO_ROWS, piece_cols(i)], preferred_element_type=F32),
               lambda v, i, band: v + x_f32[band.start:band.start + BAND],
               stage_p, r1, stage_h, r2, full1, p_s, p_r, h_s, h_r, f_s, f_r, g_s, g_r)
    first.wait_send()
    second.wait_send()
    d0_cp.start()

    sq = jnp.zeros((ROWS, 1), F32)
    for i in range(8):
        sq += jnp.sum(jnp.square(full1[i]), axis=-1, keepdims=True)
    inv = lax.rsqrt(sq / DIM + 1e-5)
    blocks = PIECE // HD
    scaled_norm(lambda i: full1[i // blocks, :, (i % blocks) * HD:(i % blocks + 1) * HD], inv, gain_ref, n_buf)

    for cp in g_cps + u_cps:
        cp.wait()
    skip = s * FFN_SHARD - start

    def hidden(j, shift):
        at = pl.ds(pl.multiple_of(j * 256, 256), 256)
        to = pl.ds(pl.multiple_of(j * 256 + shift, 256), 256)
        gate = jnp.dot(n_buf[...], g_buf[:, at], preferred_element_type=F32)
        up = jnp.dot(n_buf[...], u_buf[:, at], preferred_element_type=F32)
        act = gate / (1.0 + jnp.exp(-gate)) * up
        col = lax.broadcasted_iota(jnp.int32, (ROWS, 256), 1) + (j * 256 + shift)
        a_buf[:, to] = jnp.where(col >= skip, act, 0.0).astype(BF16)
        return 0

    tail_cps = [pltpu.make_async_copy(src.at[:, last], buf.at[:, pl.ds(0, 256)], sem_w.at[9 + i])
                for i, (src, buf) in enumerate(((wg, g_buf), (wu, u_buf)))]
    lax.fori_loop(0, 1, lambda j, carry: hidden(j, 0), 0)
    for cp in tail_cps:
        cp.start()
    lax.fori_loop(1, HELD // 256, lambda j, carry: hidden(j, 0), 0)
    for cp in tail_cps:
        cp.wait()
    hidden(0, HELD)

    d_cp.wait()
    d0_cp.wait()

    def down(i):
        at = piece_cols(i)
        return (jnp.dot(a_buf[:, :D_FIRST], wo_buf[:, at], preferred_element_type=F32)
                + jnp.dot(a_buf[:, D_FIRST:], d_buf[:, at], preferred_element_type=F32))

    all_reduce(down, lambda v, i, band: v + full1[i, band],
               stage_p, r1, stage_h, r2, full1, p_s2, p_r2, h_s2, h_r2, f_s2, f_r2, g_s2, g_r2)
    for i in range(8):
        out_ref[:, i * PIECE:(i + 1) * PIECE] = full1[i].astype(BF16)


def mlp_call(op, x, gain, wo, wg, wu, wd):
    dma = pltpu.SemaphoreType.DMA

    def pieces(n):
        return pltpu.VMEM((n, ROWS, PIECE), F32)

    ar_bufs = [pieces(4), pieces(4), pieces(3), pieces(3), pieces(8)]
    ar_sems = [dma((4,)), dma((4,))] + [dma((3, N_BAND))] * 4 + [dma((4, N_BAND))] * 2
    return pl.pallas_call(
        mlp_kernel,
        out_shape=jax.ShapeDtypeStruct((ROWS, DIM), BF16),
        in_specs=[vmem()] + [hbm()] * 6,
        out_specs=vmem(),
        scratch_shapes=[
            pltpu.VMEM((D_FIRST, DIM), BF16), pltpu.VMEM((DIM, HELD), BF16),
            pltpu.VMEM((DIM, HELD), BF16), pltpu.VMEM((D_REST, DIM), BF16),
            pltpu.VMEM((2, 6, ROWS, HD), F32), pltpu.VMEM((6, ROWS, HD), F32), pltpu.VMEM((6, ROWS, HD), F32),
            pltpu.VMEM((ROWS, WO_ROWS), BF16),
        ] + ar_bufs + [
            pltpu.VMEM((ROWS, DIM), BF16), pltpu.VMEM((ROWS, FFN_SHARD), BF16),
            pltpu.VMEM((ROWS, PIECE), BF16), pltpu.VMEM((DIM // HD, HD), BF16), dma((11,)), dma((2,)), dma((2,)),
        ] + ar_sems + ar_sems,
        compiler_params=pltpu.CompilerParams(collective_id=1, has_side_effects=True, vmem_limit_bytes=52 << 20),
        name="mlp",
    )(op, x, gain, wo, wg, wu, wd)


def solution(mesh):
    half_idx = np.arange(HD // 2, dtype=np.float64)
    freq = np.repeat(1.0 / (ROPE_THETA ** (2.0 * half_idx / HD)), 2).astype(np.float32)[None, :]

    def local_step(layer_in, new_pos, k_blk, v_blk, attn_gain, w_query, w_key, w_value, w_out, mlp_gain, w_gate, w_up, w_down):
        kc = jnp.transpose(k_blk, (0, 2, 1, 3))
        vc = jnp.transpose(v_blk, (0, 2, 1, 3))
        hb = lambda a: pltpu.with_memory_space_constraint(a, pltpu.HBM)
        q, k, v, kc = qkv_call(hb(new_pos), hb(layer_in), hb(attn_gain.reshape(DIM // HD, HD)), hb(jnp.asarray(freq)),
                               w_query, w_key, w_value, kc)
        ko, vo, kn, vn, op, _ = attn_call(new_pos, q, k, v, kc, vc)
        out = mlp_call(op, hb(layer_in), hb(mlp_gain.reshape(DIM // HD, HD)), w_out, w_gate, w_up, w_down)
        back = lambda a: jnp.transpose(a, (0, 2, 1, 3))
        return out, back(ko), back(vo), jnp.transpose(kn, (1, 0, 2)), jnp.transpose(vn, (1, 0, 2))

    cache_spec = P('dp', 'sp', 'tp', None)
    new_spec = P('dp', 'tp', None)
    in_specs = (P('dp', None), P('dp'), cache_spec, cache_spec, P(None), P(None, 'tp'), P(None, 'tp'), P(None, 'tp'), P('tp', None), P(None), P(None, 'tp'), P(None, 'tp'), P('tp', None))
    out_specs = (P('dp', None), cache_spec, cache_spec, new_spec, new_spec)
    return jax.shard_map(local_step, mesh=mesh, in_specs=in_specs, out_specs=out_specs, check_vma=False)
```

```python
import functools

import jax
import jax.numpy as jnp
import numpy as np
from jax import lax
from jax.experimental import pallas as pl
from jax.experimental.pallas import tpu as pltpu
from jax.sharding import PartitionSpec as P

ROPE_THETA = 1000000
MESH = pl.DeviceIdType.MESH
F32 = jnp.float32
BF16 = jnp.bfloat16
NEG = float(np.finfo(np.float32).min)

ROWS = 32
DIM = 5120
HEADS = 20
HD = 128
SLOTS = 128
SHARD = 640
PADH = 24
FFN_SHARD = 1792
FFN_LOC = 6912
HELD = 1536


def vmem():
    return pl.BlockSpec(memory_space=pltpu.VMEM)


def smem():
    return pl.BlockSpec(memory_space=pltpu.SMEM)


def hbm():
    return pl.BlockSpec(memory_space=pltpu.HBM)


def remote(src, dst, send_sem, recv_sem, device):
    return pltpu.make_async_remote_copy(src_ref=src, dst_ref=dst, send_sem=send_sem, recv_sem=recv_sem,
                                        device_id=device, device_id_type=MESH)


def enter_barrier(partners):
    barrier = pltpu.get_barrier_semaphore()
    for partner in partners:
        pl.semaphore_signal(barrier, inc=1, device_id=partner, device_id_type=MESH)
    pl.semaphore_wait(barrier, len(partners))


def scaled_norm(block, inv, gain_ref, n_buf):
    gain = gain_ref[...].astype(F32)
    for i in range(DIM // HD):
        n_buf[:, i * HD:(i + 1) * HD] = (block(i) * inv * gain[i:i + 1, :]).astype(BF16)


QK_CH = 4
KC_ROWS = 2
WINDOW = 4


def qkv_kernel(pos_hbm, x_hbm, gain_hbm, freq_hbm, wq, wk, wv, kc, q_out, k_out, v_out, kc_out,
               pos_ref, x_ref, gain_ref, freq_ref, w_buf, n_buf, pieces,
               sem_in, sem_kc, sem_w, d2d_s, d2d_r, ici_s, ici_r, fwd_s, fwd_r):
    s = lax.axis_index("sp")
    c = lax.rem(s, 2)
    xc = s // 2
    core_peer = 2 * xc + (1 - c)
    x_peer = 2 * (1 - xc) + c

    col = pl.multiple_of(s * SHARD, SHARD)
    rows = DIM // QK_CH

    def weight_copy(m, src, i):
        r = pl.ds(i * rows, rows)
        return pltpu.make_async_copy(src.at[r, pl.ds(col, SHARD)], w_buf.at[m, r, :], sem_w.at[m, i])

    weights = [[weight_copy(m, src, i) for i in range(QK_CH)] for m, src in enumerate((wk, wv, wq))]
    small = [pltpu.make_async_copy(a, b, sem_in.at[i]) for i, (a, b) in enumerate(
        ((x_hbm, x_ref), (gain_hbm, gain_ref), (pos_hbm, pos_ref), (freq_hbm, freq_ref)))]
    cache = [pltpu.make_async_copy(kc.at[pl.ds(i * KC_ROWS, KC_ROWS)], kc_out.at[pl.ds(i * KC_ROWS, KC_ROWS)],
                                   sem_kc.at[i]) for i in range(ROWS // KC_ROWS)]
    stream = weights[0] + weights[1] + weights[2] + cache
    for cp in small + stream[:WINDOW]:
        cp.start()
    pending = stream[WINDOW:]
    for cp in small:
        cp.wait()

    x = x_ref[...].astype(F32)
    mean_sq = jnp.mean(jnp.square(x), axis=-1, keepdims=True)
    scaled_norm(lambda i: x_ref[:, i * HD:(i + 1) * HD].astype(F32), lax.rsqrt(mean_sq + 1e-5), gain_ref, n_buf)

    row_id = lax.broadcasted_iota(jnp.int32, (ROWS, HD), 0)
    lane = lax.broadcasted_iota(jnp.int32, (ROWS, HD), 1)
    pos = jnp.zeros((ROWS, HD), jnp.int32)
    for r in range(ROWS):
        pos = jnp.where(row_id == r, pos_ref[r], pos)
    angle = pos.astype(F32) * freq_ref[...]
    cos_a = jnp.cos(angle)
    even = lax.rem(lane, 2) == 0
    sin_a = jnp.where(even, -jnp.sin(angle), jnp.sin(angle))

    def rope(v):
        swapped = jnp.where(even, pltpu.roll(v, HD - 1, 1), pltpu.roll(v, 1, 1))
        return v * cos_a + swapped * sin_a

    enter_barrier([{"sp": core_peer}, {"sp": x_peer}])

    d2d, ici = [], []
    for m in range(3):
        acc = jnp.zeros((ROWS, SHARD), F32)
        for i in range(QK_CH):
            weights[m][i].wait()
            if pending:
                pending.pop(0).start()
            acc += jnp.dot(n_buf[:, i * rows:(i + 1) * rows], w_buf[m, i * rows:(i + 1) * rows, :],
                           preferred_element_type=F32)
        for h in range(SHARD // HD):
            part = acc[:, h * HD:(h + 1) * HD]
            pieces[m, s, :, h * HD:(h + 1) * HD] = part if m == 1 else rope(part)
        mine = pieces.at[m, s]
        ici.append(remote(mine, mine, ici_s.at[m], ici_r.at[m], {"sp": x_peer}))
        d2d.append(remote(mine, mine, d2d_s.at[m], d2d_r.at[m], {"sp": core_peer}))
        ici[m].start()
        d2d[m].start()
    for cp in pending:
        cp.start()

    fwd = []
    for m in range(3):
        ici[m].wait_recv()
        theirs = pieces.at[m, x_peer]
        fwd.append(remote(theirs, theirs, fwd_s.at[m], fwd_r.at[m], {"sp": core_peer}))
        fwd[m].start()
    for m, out in enumerate((k_out, v_out, q_out)):
        d2d[m].wait()
        fwd[m].wait()
        ici[m].wait_send()
        for i in range(4):
            out[:, i * SHARD:(i + 1) * SHARD] = pieces[m, i]
    for cp in cache:
        cp.wait()


def qkv_call(pos, x, gain, freq, wq, wk, wv, kc):
    out = jax.ShapeDtypeStruct((ROWS, HEADS * HD), F32)
    dma = pltpu.SemaphoreType.DMA
    return pl.pallas_call(
        qkv_kernel,
        out_shape=(out, out, out, jax.ShapeDtypeStruct(kc.shape, kc.dtype)),
        in_specs=[hbm()] * 8,
        out_specs=(vmem(), vmem(), vmem(), vmem()),
        scratch_shapes=[
            pltpu.SMEM((ROWS,), jnp.int32), pltpu.VMEM((ROWS, DIM), BF16), pltpu.VMEM((DIM // HD, HD), BF16),
            pltpu.VMEM((1, HD), F32), pltpu.VMEM((3, DIM, SHARD), BF16), pltpu.VMEM((ROWS, DIM), BF16),
            pltpu.VMEM((3, 4, ROWS, SHARD), F32),
            dma((4,)), dma((ROWS // KC_ROWS,)), dma((3, QK_CH)),
        ] + [dma((3,))] * 6,
        compiler_params=pltpu.CompilerParams(collective_id=0, has_side_effects=True, vmem_limit_bytes=28 << 20),
        name="qkv",
    )(pos, x, gain, freq, wq, wk, wv, kc)


RING = 18
AHEAD = 12
STEP_ROWS = 2


def attn_kernel(pos_ref, q_ref, k_ref, v_ref, kin, vc, ko, vo, kn_ref, vn_ref, op_ref, kbuf,
                vbuf, q3, k3, v3, o3, w3, st, sem_vi, sem_ko, sem_vo):
    s = lax.axis_index("sp")
    base = s * SLOTS

    def v_in(b, slot):
        return pltpu.make_async_copy(vc.at[b], vbuf.at[slot], sem_vi.at[slot])

    def v_out(b, slot):
        return pltpu.make_async_copy(vbuf.at[slot], vo.at[b], sem_vo.at[slot])

    def k_out(b):
        return pltpu.make_async_copy(kbuf.at[b], ko.at[b], sem_ko.at[b])

    for b in range(AHEAD):
        v_in(b, b).start()

    for h in range(HEADS):
        sl = slice(h * HD, (h + 1) * HD)
        q3[pl.ds(h, ROWS, stride=PADH), :] = q_ref[:, sl]
        k3[pl.ds(h, ROWS, stride=PADH), :] = k_ref[:, sl]
        v3[pl.ds(h, ROWS, stride=PADH), :] = v_ref[:, sl]
        kn_ref[h] = k_ref[:, sl].astype(BF16)
        vn_ref[h] = v_ref[:, sl].astype(BF16)
    st[...] = jnp.zeros_like(st)

    lane = lax.broadcasted_iota(jnp.int32, (8, HD), 1)
    sub = lax.broadcasted_iota(jnp.int32, (8, HD), 0)
    even = lax.rem(sub, 2) == 0
    scale = HD ** -0.5

    def patch(b, buf, at, new):
        rel = pos_ref[b] - base

        @pl.when(jnp.logical_and(rel >= 0, rel < SLOTS))
        def _():
            start = pl.multiple_of((rel // 16) * 16, 16)
            here = lax.broadcasted_iota(jnp.int32, (16, HD), 0) == rel - start
            for h in range(HEADS):
                row = jnp.broadcast_to(new[pl.ds(b * PADH + h, 1), :], (16, HD))
                old = buf[at, h, pl.ds(start, 16), :].astype(F32)
                buf[at, h, pl.ds(start, 16), :] = jnp.where(here, row, old).astype(BF16)

    def pair_rows(v):
        return jnp.concatenate([jnp.where(even, v, 0.0), jnp.where(even, 0.0, v)], axis=1).astype(BF16)

    def pick(parts):
        out = parts[-1][:, HD:]
        for i in range(len(parts) - 1, -1, -1):
            if i < len(parts) - 1:
                out = jnp.where(sub < 4 * i + 4, parts[i][:, HD:], out)
            out = jnp.where(sub < 4 * i + 2, parts[i][:, :HD], out)
        return out

    def scores(b, j):
        rel = pos_ref[b] - base
        valid = lane <= rel
        at_b = lane == b
        for g in range(0, HEADS, 8):
            row0 = pl.multiple_of(b * PADH + g, 8)
            qg = pair_rows(q3[pl.ds(row0, 8), :])
            parts = []
            for i in range(min(8, HEADS - g) // 4):
                h = g + 4 * i
                tile = jnp.concatenate([
                    jnp.concatenate([kbuf[b, h], kbuf[b, h + 1]], axis=1),
                    jnp.concatenate([kbuf[b, h + 2], kbuf[b, h + 3]], axis=1)], axis=0)
                parts.append(lax.dot_general(qg, tile, (((1,), (1,)), ((), ())), preferred_element_type=F32))
            sc = jnp.where(valid, pick(parts) * scale, NEG)
            top = jnp.max(sc, axis=-1, keepdims=True)
            w = jnp.where(valid, jnp.exp(sc - top), 0.0)
            total = jnp.sum(w, axis=-1, keepdims=True)
            w3[j * PADH + g:j * PADH + g + 8, :] = w
            st[g:g + 8, :] = jnp.where(at_b, top, st[g:g + 8, :])
            st[64 + g:64 + g + 8, :] = jnp.where(at_b, total, st[64 + g:64 + g + 8, :])

    def values(b, j, slot):
        for g in range(0, HEADS, 8):
            wg = pair_rows(w3[j * PADH + g:j * PADH + g + 8, :])
            parts = []
            for i in range(min(8, HEADS - g) // 4):
                h = g + 4 * i
                tile = jnp.concatenate([
                    jnp.concatenate([vbuf[slot, h], vbuf[slot, h + 2]], axis=1),
                    jnp.concatenate([vbuf[slot, h + 1], vbuf[slot, h + 3]], axis=1)], axis=0)
                parts.append(jnp.dot(wg, tile, preferred_element_type=F32))
            o3[pl.ds(pl.multiple_of(b * PADH + g, 8), 8), :] = pick(parts)

    def step(i, carry):
        rows = [i * STEP_ROWS + j for j in range(STEP_ROWS)]
        for b in rows:
            nxt = b + AHEAD
            nslot = lax.rem(nxt, RING)

            @pl.when(nxt < ROWS)
            def _():
                @pl.when(nxt >= RING)
                def _():
                    v_out(nxt - RING, nslot).wait()
                v_in(nxt, nslot).start()
        for b in rows:
            v_in(b, lax.rem(b, RING)).wait()
        for b in rows:
            patch(b, vbuf, lax.rem(b, RING), v3)
        for b in rows:
            k_out(b).start()
        for j, b in enumerate(rows):
            scores(b, j)

        @pl.when(pos_ref[0] >= 0)
        def _():
            for j, b in enumerate(rows):
                values(b, j, lax.rem(b, RING))

        for b in rows:
            v_out(b, lax.rem(b, RING)).start()

            @pl.when(b + STEP_ROWS < ROWS)
            def _():
                patch(b + STEP_ROWS, kbuf, b + STEP_ROWS, k3)
        return carry

    for b in range(STEP_ROWS):
        patch(b, kbuf, b, k3)
    lax.fori_loop(0, ROWS // STEP_ROWS, step, 0)

    stats = jnp.transpose(st[...])[:ROWS, :]
    for c in range(2):
        for xc in range(2):
            o = 2 * xc + c
            for j in range(5):
                op_ref[2 * c + xc, j] = o3[pl.ds(5 * o + j, ROWS, stride=PADH), :]
            op_ref[2 * c + xc, 5] = pltpu.roll(stats, HD - 5 * o, 1) if o else stats
    for b in range(ROWS - RING, ROWS):
        v_out(b, b % RING).wait()

    def drain(b, carry):
        k_out(b).wait()
        return carry

    lax.fori_loop(0, ROWS, drain, 0)


def attn_call(pos, q, k, v, kc, vc):
    cache = jax.ShapeDtypeStruct((ROWS, HEADS, SLOTS, HD), BF16)
    new = jax.ShapeDtypeStruct((HEADS, ROWS, HD), BF16)
    part = jax.ShapeDtypeStruct((4, 6, ROWS, HD), F32)
    dma = pltpu.SemaphoreType.DMA
    flat = pltpu.VMEM((ROWS * PADH, HD), F32)
    return pl.pallas_call(
        attn_kernel,
        out_shape=(cache, cache, new, new, part, cache),
        in_specs=[smem(), vmem(), vmem(), vmem(), vmem(), hbm()],
        out_specs=(hbm(), hbm(), vmem(), vmem(), vmem(), vmem()),
        input_output_aliases={4: 5},
        scratch_shapes=[
            pltpu.VMEM((RING, HEADS, SLOTS, HD), BF16),
            flat, flat, flat, flat, pltpu.VMEM((STEP_ROWS * PADH, HD), F32), pltpu.VMEM((HD, HD), F32),
            dma((RING,)), dma((ROWS,)), dma((RING,)),
        ],
        compiler_params=pltpu.CompilerParams(vmem_limit_bytes=20 << 20),
        name="attn",
    )(pos, q, k, v, kc, vc)


WO_ROWS = 640
D_FIRST = 768
D_REST = FFN_SHARD - D_FIRST
PIECE = 640
BAND = 16
N_BAND = ROWS // BAND


def combine(a_o, a_st, b_o, b_st):
    lane = lax.broadcasted_iota(jnp.int32, (ROWS, HD), 1)
    is_max = lane < 64
    top = jnp.maximum(a_st, b_st)
    fa = jnp.exp(jnp.where(is_max, a_st - top, 0.0))
    fb = jnp.exp(jnp.where(is_max, b_st - top, 0.0))
    total = pltpu.roll(fa, 64, 1) * a_st + pltpu.roll(fb, 64, 1) * b_st
    out = [fa[:, j:j + 1] * a_o[j] + fb[:, j:j + 1] * b_o[j] for j in range(5)]
    return out, jnp.where(is_max, top, total)


def mlp_kernel(op_ref, x, gain, wo, wg, wu, wd, out_ref,
               wo_buf, g_buf, u_buf, d_buf, rs1, z, rs2, attn_buf,
               stage_p, r1, stage_h, r2, full1, n_buf, a_buf, x_ref, gain_ref,
               sem_w, rs_s, rs_r, p_s, p_r, h_s, h_r, f_s, f_r, g_s, g_r,
               p_s2, p_r2, h_s2, h_r2, f_s2, f_r2, g_s2, g_r2):
    s = lax.axis_index("sp")
    t = lax.axis_index("tp")
    c = lax.rem(s, 2)
    xc = s // 2
    ot, ox, oc = 1 - t, 1 - xc, 1 - c
    core_dev = {"tp": t, "sp": 2 * xc + oc}
    chips = [(t, xc), (t, ox), (ot, xc), (ot, ox)]
    devs = [{"tp": ct, "sp": 2 * cx + c} for ct, cx in chips]
    chip_id = [2 * ct + cx for ct, cx in chips]

    wo_row = pl.multiple_of(s * WO_ROWS, WO_ROWS)
    start = pl.multiple_of(jnp.minimum(s * FFN_SHARD, FFN_LOC - FFN_SHARD), 256)
    half = DIM // 2
    held = pl.ds(start, HELD)
    last = pl.ds(start + HELD, FFN_SHARD - HELD)

    wo_cp = pltpu.make_async_copy(wo.at[pl.ds(wo_row, WO_ROWS), :], wo_buf.at[pl.ds(0, WO_ROWS), :], sem_w.at[0])
    g_cps = [pltpu.make_async_copy(wg.at[pl.ds(i * half, half), held], g_buf.at[pl.ds(i * half, half), :],
                                   sem_w.at[1 + i]) for i in range(2)]
    u_cps = [pltpu.make_async_copy(wu.at[pl.ds(i * half, half), held], u_buf.at[pl.ds(i * half, half), :],
                                   sem_w.at[3 + i]) for i in range(2)]
    d_cp = pltpu.make_async_copy(wd.at[pl.ds(start + D_FIRST, D_REST), :], d_buf, sem_w.at[5])
    d0_cp = pltpu.make_async_copy(wd.at[pl.ds(start, D_FIRST), :], wo_buf, sem_w.at[6])
    own_piece = pl.ds(pl.multiple_of((c * 4 + chip_id[0]) * PIECE, PIECE), PIECE)
    x_cp = pltpu.make_async_copy(x.at[:, own_piece], x_ref, sem_w.at[7])
    gain_cp = pltpu.make_async_copy(gain, gain_ref, sem_w.at[8])
    for cp in (x_cp, gain_cp, wo_cp, g_cps[0]):
        cp.start()
    enter_barrier([core_dev] + devs[1:])

    first = remote(op_ref.at[pl.ds(oc * 2, 2)], rs1, rs_s.at[0], rs_r.at[0], core_dev)
    first.start()
    first.wait_recv()

    def merge(i):
        mine = 2 * c + i
        return combine([op_ref[mine, j] for j in range(5)], op_ref[mine, 5],
                       [rs1[i, j] for j in range(5)], rs1[i, 5])

    o_out, st_out = merge(ox)
    for j in range(5):
        z[j] = o_out[j]
    z[5] = st_out
    second = remote(z, rs2, rs_s.at[1], rs_r.at[1], devs[1])
    second.start()
    o_own, st_own = merge(xc)
    for cp in (x_cp, gain_cp, wo_cp):
        cp.wait()
    for cp in (g_cps[1], u_cps[0], u_cps[1]):
        cp.start()
    second.wait_recv()
    o_all, st_all = combine(o_own, st_own, [rs2[j] for j in range(5)], rs2[5])
    for j in range(5):
        attn_buf[:, j * HD:(j + 1) * HD] = (o_all[j] / st_all[:, 64 + j:65 + j]).astype(BF16)

    def all_reduce(compute, finish, after, stage_p, r1, stage_h, r2, full, p_s, p_r, h_s, h_r, f_s, f_r, g_s, g_r):
        order = (3, 1, 2, 0)
        bands = [pl.ds(i * BAND, BAND) for i in range(N_BAND)]
        to_core = {}
        own, to_chip = None, {}

        def for_core(d):
            stage_p[d] = compute(oc * 4 + chip_id[d])
            to_core[d] = remote(stage_p.at[d], r1.at[d], p_s.at[d], p_r.at[d], core_dev)
            to_core[d].start()

        for_core(order[0])
        for_core(order[1])
        for n, d in enumerate(order):
            part = compute(c * 4 + chip_id[d])
            to_core[d].wait_recv()
            part = part + r1[d]
            if d:
                stage_h[d - 1] = part
                for i, band in enumerate(bands):
                    to_chip[d, i] = remote(stage_h.at[d - 1, band], r2.at[d - 1, band], h_s.at[d - 1, i],
                                           h_r.at[d - 1, i], devs[d])
                    to_chip[d, i].start()
            else:
                own = part
            if n + 2 < 4:
                for_core(order[n + 2])
        after()
        mine = c * 4 + chip_id[0]
        sends, forward = {}, {}
        for i, band in enumerate(bands):
            total = own[i * BAND:(i + 1) * BAND]
            for d in (1, 2, 3):
                to_chip[d, i].wait_recv()
                total = total + r2[d - 1, band]
            full[mine, band] = finish(total, mine, band)
            here = full.at[mine, band]
            for d in (3, 1, 2):
                sends[d, i] = remote(here, here, f_s.at[d - 1, i], f_r.at[d - 1, i], devs[d])
                sends[d, i].start()
            forward[0, i] = remote(here, here, g_s.at[0, i], g_r.at[0, i], core_dev)
            forward[0, i].start()
        for i, band in enumerate(bands):
            for d in (1, 2, 3):
                sends[d, i].wait_recv()
                piece = full.at[c * 4 + chip_id[d], band]
                forward[d, i] = remote(piece, piece, g_s.at[d, i], g_r.at[d, i], core_dev)
                forward[d, i].start()
        for cp in forward.values():
            cp.wait_recv()
        for group in (forward, sends, to_chip, to_core):
            for cp in group.values():
                cp.wait_send()

    def piece_cols(i):
        return pl.ds(pl.multiple_of(i * PIECE, PIECE), PIECE)

    d_cp.start()
    x_f32 = x_ref[...].astype(F32)
    all_reduce(lambda i: jnp.dot(attn_buf[...], wo_buf[:WO_ROWS, piece_cols(i)], preferred_element_type=F32),
               lambda v, i, band: v + x_f32[band.start:band.start + BAND], d0_cp.start,
               stage_p, r1, stage_h, r2, full1, p_s, p_r, h_s, h_r, f_s, f_r, g_s, g_r)
    first.wait_send()
    second.wait_send()

    sq = jnp.zeros((ROWS, 1), F32)
    for i in range(8):
        sq += jnp.sum(jnp.square(full1[i]), axis=-1, keepdims=True)
    inv = lax.rsqrt(sq / DIM + 1e-5)
    blocks = PIECE // HD
    scaled_norm(lambda i: full1[i // blocks, :, (i % blocks) * HD:(i % blocks + 1) * HD], inv, gain_ref, n_buf)

    for cp in g_cps + u_cps:
        cp.wait()
    skip = s * FFN_SHARD - start

    def hidden(j, shift, width):
        at = pl.ds(pl.multiple_of(j * width, 256), width)
        to = pl.ds(pl.multiple_of(j * width + shift, 256), width)
        gate = jnp.dot(n_buf[...], g_buf[:, at], preferred_element_type=F32)
        up = jnp.dot(n_buf[...], u_buf[:, at], preferred_element_type=F32)
        act = gate / (1.0 + jnp.exp(-gate)) * up
        col = lax.broadcasted_iota(jnp.int32, (ROWS, width), 1) + (j * width + shift)
        a_buf[:, to] = jnp.where(col >= skip, act, 0.0).astype(BF16)
        return 0

    tail_cps = [pltpu.make_async_copy(src.at[:, last], buf.at[:, pl.ds(0, 256)], sem_w.at[9 + i])
                for i, (src, buf) in enumerate(((wg, g_buf), (wu, u_buf)))]
    hidden(0, 0, 512)
    for cp in tail_cps:
        cp.start()
    lax.fori_loop(1, HELD // 512, lambda j, carry: hidden(j, 0, 512), 0)
    for cp in tail_cps:
        cp.wait()
    hidden(0, HELD, 256)

    d_cp.wait()
    d0_cp.wait()

    def down(i):
        at = piece_cols(i)
        return (jnp.dot(a_buf[:, :D_FIRST], wo_buf[:, at], preferred_element_type=F32)
                + jnp.dot(a_buf[:, D_FIRST:], d_buf[:, at], preferred_element_type=F32))

    all_reduce(down, lambda v, i, band: v + full1[i, band], lambda: None,
               stage_p, r1, stage_h, r2, full1, p_s2, p_r2, h_s2, h_r2, f_s2, f_r2, g_s2, g_r2)
    for i in range(8):
        out_ref[:, i * PIECE:(i + 1) * PIECE] = full1[i].astype(BF16)


def mlp_call(op, x, gain, wo, wg, wu, wd):
    dma = pltpu.SemaphoreType.DMA

    def pieces(n):
        return pltpu.VMEM((n, ROWS, PIECE), F32)

    ar_bufs = [pieces(4), pieces(4), pieces(3), pieces(3), pieces(8)]
    ar_sems = [dma((4,)), dma((4,))] + [dma((3, N_BAND))] * 4 + [dma((4, N_BAND))] * 2
    return pl.pallas_call(
        mlp_kernel,
        out_shape=jax.ShapeDtypeStruct((ROWS, DIM), BF16),
        in_specs=[vmem()] + [hbm()] * 6,
        out_specs=vmem(),
        scratch_shapes=[
            pltpu.VMEM((D_FIRST, DIM), BF16), pltpu.VMEM((DIM, HELD), BF16),
            pltpu.VMEM((DIM, HELD), BF16), pltpu.VMEM((D_REST, DIM), BF16),
            pltpu.VMEM((2, 6, ROWS, HD), F32), pltpu.VMEM((6, ROWS, HD), F32), pltpu.VMEM((6, ROWS, HD), F32),
            pltpu.VMEM((ROWS, WO_ROWS), BF16),
        ] + ar_bufs + [
            pltpu.VMEM((ROWS, DIM), BF16), pltpu.VMEM((ROWS, FFN_SHARD), BF16),
            pltpu.VMEM((ROWS, PIECE), BF16), pltpu.VMEM((DIM // HD, HD), BF16), dma((11,)), dma((2,)), dma((2,)),
        ] + ar_sems + ar_sems,
        compiler_params=pltpu.CompilerParams(collective_id=1, has_side_effects=True, vmem_limit_bytes=52 << 20),
        name="mlp",
    )(op, x, gain, wo, wg, wu, wd)


def solution(mesh):
    half_idx = np.arange(HD // 2, dtype=np.float64)
    freq = np.repeat(1.0 / (ROPE_THETA ** (2.0 * half_idx / HD)), 2).astype(np.float32)[None, :]

    def local_step(layer_in, new_pos, k_blk, v_blk, attn_gain, w_query, w_key, w_value, w_out, mlp_gain, w_gate, w_up, w_down):
        kc = jnp.transpose(k_blk, (0, 2, 1, 3))
        vc = jnp.transpose(v_blk, (0, 2, 1, 3))
        hb = lambda a: pltpu.with_memory_space_constraint(a, pltpu.HBM)
        q, k, v, kc = qkv_call(hb(new_pos), hb(layer_in), hb(attn_gain.reshape(DIM // HD, HD)), hb(jnp.asarray(freq)),
                               w_query, w_key, w_value, kc)
        ko, vo, kn, vn, op, _ = attn_call(new_pos, q, k, v, kc, vc)
        out = mlp_call(op, hb(layer_in), hb(mlp_gain.reshape(DIM // HD, HD)), w_out, w_gate, w_up, w_down)
        back = lambda a: jnp.transpose(a, (0, 2, 1, 3))
        return out, back(ko), back(vo), jnp.transpose(kn, (1, 0, 2)), jnp.transpose(vn, (1, 0, 2))

    cache_spec = P('dp', 'sp', 'tp', None)
    new_spec = P('dp', 'tp', None)
    in_specs = (P('dp', None), P('dp'), cache_spec, cache_spec, P(None), P(None, 'tp'), P(None, 'tp'), P(None, 'tp'), P('tp', None), P(None), P(None, 'tp'), P(None, 'tp'), P('tp', None))
    out_specs = (P('dp', None), cache_spec, cache_spec, new_spec, new_spec)
    return jax.shard_map(local_step, mesh=mesh, in_specs=in_specs, out_specs=out_specs, check_vma=False)
```

```python
import functools

import jax
import jax.numpy as jnp
import numpy as np
from jax import lax
from jax.experimental import pallas as pl
from jax.experimental.pallas import tpu as pltpu
from jax.sharding import PartitionSpec as P

ROPE_THETA = 1000000
MESH = pl.DeviceIdType.MESH
F32 = jnp.float32
BF16 = jnp.bfloat16
NEG = float(np.finfo(np.float32).min)

ROWS = 32
DIM = 5120
HEADS = 20
HD = 128
SLOTS = 128
SHARD = 640
PADH = 24
FFN_SHARD = 1792
FFN_LOC = 6912
HELD = 1536


def vmem():
    return pl.BlockSpec(memory_space=pltpu.VMEM)


def smem():
    return pl.BlockSpec(memory_space=pltpu.SMEM)


def hbm():
    return pl.BlockSpec(memory_space=pltpu.HBM)


def remote(src, dst, send_sem, recv_sem, device):
    return pltpu.make_async_remote_copy(src_ref=src, dst_ref=dst, send_sem=send_sem, recv_sem=recv_sem,
                                        device_id=device, device_id_type=MESH)


def greet(partners):
    barrier = pltpu.get_barrier_semaphore()
    for partner in partners:
        pl.semaphore_signal(barrier, inc=1, device_id=partner, device_id_type=MESH)
    return lambda: pl.semaphore_wait(barrier, len(partners))


def scaled_norm(block, inv, gain_ref, n_buf):
    gain = gain_ref[...].astype(F32)
    for i in range(DIM // HD):
        n_buf[:, i * HD:(i + 1) * HD] = (block(i) * inv * gain[i:i + 1, :]).astype(BF16)


QK_CH = 4
KC_ROWS = 2
WINDOW = 4


def qkv_kernel(pos_hbm, x_hbm, gain_hbm, freq_hbm, wq, wk, wv, kc, q_out, k_out, v_out, kc_out,
               pos_ref, x_ref, gain_ref, freq_ref, w_buf, n_buf, pieces,
               sem_in, sem_kc, sem_w, d2d_s, d2d_r, ici_s, ici_r, fwd_s, fwd_r):
    s = lax.axis_index("sp")
    c = lax.rem(s, 2)
    xc = s // 2
    core_peer = 2 * xc + (1 - c)
    x_peer = 2 * (1 - xc) + c

    all_here = greet([{"sp": core_peer}, {"sp": x_peer}])
    col = pl.multiple_of(s * SHARD, SHARD)
    rows = DIM // QK_CH

    def weight_copy(m, src, i):
        r = pl.ds(i * rows, rows)
        return pltpu.make_async_copy(src.at[r, pl.ds(col, SHARD)], w_buf.at[m, r, :], sem_w.at[m, i])

    weights = [[weight_copy(m, src, i) for i in range(QK_CH)] for m, src in enumerate((wk, wv, wq))]
    small = [pltpu.make_async_copy(a, b, sem_in.at[i]) for i, (a, b) in enumerate(
        ((x_hbm, x_ref), (gain_hbm, gain_ref), (pos_hbm, pos_ref), (freq_hbm, freq_ref)))]
    cache = [pltpu.make_async_copy(kc.at[pl.ds(i * KC_ROWS, KC_ROWS)], kc_out.at[pl.ds(i * KC_ROWS, KC_ROWS)],
                                   sem_kc.at[i]) for i in range(ROWS // KC_ROWS)]
    stream = weights[0] + weights[1] + weights[2] + cache
    for cp in small + stream[:WINDOW]:
        cp.start()
    pending = stream[WINDOW:]
    for cp in small:
        cp.wait()

    x = x_ref[...].astype(F32)
    mean_sq = jnp.mean(jnp.square(x), axis=-1, keepdims=True)
    scaled_norm(lambda i: x_ref[:, i * HD:(i + 1) * HD].astype(F32), lax.rsqrt(mean_sq + 1e-5), gain_ref, n_buf)

    row_id = lax.broadcasted_iota(jnp.int32, (ROWS, HD), 0)
    lane = lax.broadcasted_iota(jnp.int32, (ROWS, HD), 1)
    pos = jnp.zeros((ROWS, HD), jnp.int32)
    for r in range(ROWS):
        pos = jnp.where(row_id == r, pos_ref[r], pos)
    angle = pos.astype(F32) * freq_ref[...]
    cos_a = jnp.cos(angle)
    even = lax.rem(lane, 2) == 0
    sin_a = jnp.where(even, -jnp.sin(angle), jnp.sin(angle))

    def rope(v):
        swapped = jnp.where(even, pltpu.roll(v, HD - 1, 1), pltpu.roll(v, 1, 1))
        return v * cos_a + swapped * sin_a

    d2d, ici = [], []
    for m in range(3):
        acc = jnp.zeros((ROWS, SHARD), F32)
        for i in range(QK_CH):
            weights[m][i].wait()
            if pending:
                pending.pop(0).start()
            acc += jnp.dot(n_buf[:, i * rows:(i + 1) * rows], w_buf[m, i * rows:(i + 1) * rows, :],
                           preferred_element_type=F32)
        for h in range(SHARD // HD):
            part = acc[:, h * HD:(h + 1) * HD]
            pieces[m, s, :, h * HD:(h + 1) * HD] = part if m == 1 else rope(part)
        if m == 0:
            all_here()
        mine = pieces.at[m, s]
        ici.append(remote(mine, mine, ici_s.at[m], ici_r.at[m], {"sp": x_peer}))
        d2d.append(remote(mine, mine, d2d_s.at[m], d2d_r.at[m], {"sp": core_peer}))
        ici[m].start()
        d2d[m].start()
    for cp in pending:
        cp.start()

    fwd = []
    for m in range(3):
        ici[m].wait_recv()
        theirs = pieces.at[m, x_peer]
        fwd.append(remote(theirs, theirs, fwd_s.at[m], fwd_r.at[m], {"sp": core_peer}))
        fwd[m].start()
    for m, out in enumerate((k_out, v_out, q_out)):
        d2d[m].wait()
        fwd[m].wait()
        ici[m].wait_send()
        for i in range(4):
            out[:, i * SHARD:(i + 1) * SHARD] = pieces[m, i]
    for cp in cache:
        cp.wait()


def qkv_call(pos, x, gain, freq, wq, wk, wv, kc):
    out = jax.ShapeDtypeStruct((ROWS, HEADS * HD), F32)
    dma = pltpu.SemaphoreType.DMA
    return pl.pallas_call(
        qkv_kernel,
        out_shape=(out, out, out, jax.ShapeDtypeStruct(kc.shape, kc.dtype)),
        in_specs=[hbm()] * 8,
        out_specs=(vmem(), vmem(), vmem(), vmem()),
        scratch_shapes=[
            pltpu.SMEM((ROWS,), jnp.int32), pltpu.VMEM((ROWS, DIM), BF16), pltpu.VMEM((DIM // HD, HD), BF16),
            pltpu.VMEM((1, HD), F32), pltpu.VMEM((3, DIM, SHARD), BF16), pltpu.VMEM((ROWS, DIM), BF16),
            pltpu.VMEM((3, 4, ROWS, SHARD), F32),
            dma((4,)), dma((ROWS // KC_ROWS,)), dma((3, QK_CH)),
        ] + [dma((3,))] * 6,
        compiler_params=pltpu.CompilerParams(collective_id=0, has_side_effects=True, vmem_limit_bytes=28 << 20),
        name="qkv",
    )(pos, x, gain, freq, wq, wk, wv, kc)


RING = 18
AHEAD = 12
STEP_ROWS = 2


def attn_kernel(pos_ref, q_ref, k_ref, v_ref, kin, vc, ko, vo, kn_ref, vn_ref, op_ref, kbuf,
                vbuf, q3, k3, v3, o3, w3, st, sem_vi, sem_ko, sem_vo):
    s = lax.axis_index("sp")
    base = s * SLOTS

    def v_in(b, slot):
        return pltpu.make_async_copy(vc.at[b], vbuf.at[slot], sem_vi.at[slot])

    def v_out(b, slot):
        return pltpu.make_async_copy(vbuf.at[slot], vo.at[b], sem_vo.at[slot])

    def k_out(b):
        return pltpu.make_async_copy(kbuf.at[b], ko.at[b], sem_ko.at[b])

    for b in range(AHEAD):
        v_in(b, b).start()

    for h in range(HEADS):
        sl = slice(h * HD, (h + 1) * HD)
        q3[pl.ds(h, ROWS, stride=PADH), :] = q_ref[:, sl]
        k3[pl.ds(h, ROWS, stride=PADH), :] = k_ref[:, sl]
        v3[pl.ds(h, ROWS, stride=PADH), :] = v_ref[:, sl]
        kn_ref[h] = k_ref[:, sl].astype(BF16)
        vn_ref[h] = v_ref[:, sl].astype(BF16)
    st[...] = jnp.zeros_like(st)

    lane = lax.broadcasted_iota(jnp.int32, (8, HD), 1)
    sub = lax.broadcasted_iota(jnp.int32, (8, HD), 0)
    even = lax.rem(sub, 2) == 0
    scale = HD ** -0.5

    def patch(b, buf, at, new):
        rel = pos_ref[b] - base

        @pl.when(jnp.logical_and(rel >= 0, rel < SLOTS))
        def _():
            start = pl.multiple_of((rel // 16) * 16, 16)
            here = lax.broadcasted_iota(jnp.int32, (16, HD), 0) == rel - start
            for h in range(HEADS):
                row = jnp.broadcast_to(new[pl.ds(b * PADH + h, 1), :], (16, HD))
                old = buf[at, h, pl.ds(start, 16), :].astype(F32)
                buf[at, h, pl.ds(start, 16), :] = jnp.where(here, row, old).astype(BF16)

    def pair_rows(v):
        return jnp.concatenate([jnp.where(even, v, 0.0), jnp.where(even, 0.0, v)], axis=1).astype(BF16)

    def pick(parts):
        out = parts[-1][:, HD:]
        for i in range(len(parts) - 1, -1, -1):
            if i < len(parts) - 1:
                out = jnp.where(sub < 4 * i + 4, parts[i][:, HD:], out)
            out = jnp.where(sub < 4 * i + 2, parts[i][:, :HD], out)
        return out

    def scores(b, j):
        rel = pos_ref[b] - base
        valid = lane <= rel
        at_b = lane == b
        for g in range(0, HEADS, 8):
            row0 = pl.multiple_of(b * PADH + g, 8)
            qg = pair_rows(q3[pl.ds(row0, 8), :])
            parts = []
            for i in range(min(8, HEADS - g) // 4):
                h = g + 4 * i
                tile = jnp.concatenate([
                    jnp.concatenate([kbuf[b, h], kbuf[b, h + 1]], axis=1),
                    jnp.concatenate([kbuf[b, h + 2], kbuf[b, h + 3]], axis=1)], axis=0)
                parts.append(lax.dot_general(qg, tile, (((1,), (1,)), ((), ())), preferred_element_type=F32))
            sc = jnp.where(valid, pick(parts) * scale, NEG)
            top = jnp.max(sc, axis=-1, keepdims=True)
            w = jnp.where(valid, jnp.exp(sc - top), 0.0)
            total = jnp.sum(w, axis=-1, keepdims=True)
            w3[j * PADH + g:j * PADH + g + 8, :] = w
            st[g:g + 8, :] = jnp.where(at_b, top, st[g:g + 8, :])
            st[64 + g:64 + g + 8, :] = jnp.where(at_b, total, st[64 + g:64 + g + 8, :])

    def values(b, j, slot):
        for g in range(0, HEADS, 8):
            wg = pair_rows(w3[j * PADH + g:j * PADH + g + 8, :])
            parts = []
            for i in range(min(8, HEADS - g) // 4):
                h = g + 4 * i
                tile = jnp.concatenate([
                    jnp.concatenate([vbuf[slot, h], vbuf[slot, h + 2]], axis=1),
                    jnp.concatenate([vbuf[slot, h + 1], vbuf[slot, h + 3]], axis=1)], axis=0)
                parts.append(jnp.dot(wg, tile, preferred_element_type=F32))
            o3[pl.ds(pl.multiple_of(b * PADH + g, 8), 8), :] = pick(parts)

    def step(i, carry):
        rows = [i * STEP_ROWS + j for j in range(STEP_ROWS)]
        for b in rows:
            nxt = b + AHEAD
            nslot = lax.rem(nxt, RING)

            @pl.when(nxt < ROWS)
            def _():
                @pl.when(nxt >= RING)
                def _():
                    v_out(nxt - RING, nslot).wait()
                v_in(nxt, nslot).start()
        for b in rows:
            v_in(b, lax.rem(b, RING)).wait()
        for b in rows:
            patch(b, vbuf, lax.rem(b, RING), v3)
        for b in rows:
            k_out(b).start()
        for j, b in enumerate(rows):
            scores(b, j)

        @pl.when(pos_ref[0] >= 0)
        def _():
            for j, b in enumerate(rows):
                values(b, j, lax.rem(b, RING))

        for b in rows:
            v_out(b, lax.rem(b, RING)).start()

            @pl.when(b + STEP_ROWS < ROWS)
            def _():
                patch(b + STEP_ROWS, kbuf, b + STEP_ROWS, k3)
        return carry

    for b in range(STEP_ROWS):
        patch(b, kbuf, b, k3)
    lax.fori_loop(0, ROWS // STEP_ROWS, step, 0)

    stats = jnp.transpose(st[...])[:ROWS, :]
    for c in range(2):
        for xc in range(2):
            o = 2 * xc + c
            for j in range(5):
                op_ref[2 * c + xc, j] = o3[pl.ds(5 * o + j, ROWS, stride=PADH), :]
            op_ref[2 * c + xc, 5] = pltpu.roll(stats, HD - 5 * o, 1) if o else stats
    for b in range(ROWS - RING, ROWS):
        v_out(b, b % RING).wait()

    def drain(b, carry):
        k_out(b).wait()
        return carry

    lax.fori_loop(0, ROWS, drain, 0)


def attn_call(pos, q, k, v, kc, vc):
    cache = jax.ShapeDtypeStruct((ROWS, HEADS, SLOTS, HD), BF16)
    new = jax.ShapeDtypeStruct((HEADS, ROWS, HD), BF16)
    part = jax.ShapeDtypeStruct((4, 6, ROWS, HD), F32)
    dma = pltpu.SemaphoreType.DMA
    flat = pltpu.VMEM((ROWS * PADH, HD), F32)
    return pl.pallas_call(
        attn_kernel,
        out_shape=(cache, cache, new, new, part, cache),
        in_specs=[smem(), vmem(), vmem(), vmem(), vmem(), hbm()],
        out_specs=(hbm(), hbm(), vmem(), vmem(), vmem(), vmem()),
        input_output_aliases={4: 5},
        scratch_shapes=[
            pltpu.VMEM((RING, HEADS, SLOTS, HD), BF16),
            flat, flat, flat, flat, pltpu.VMEM((STEP_ROWS * PADH, HD), F32), pltpu.VMEM((HD, HD), F32),
            dma((RING,)), dma((ROWS,)), dma((RING,)),
        ],
        compiler_params=pltpu.CompilerParams(vmem_limit_bytes=20 << 20),
        name="attn",
    )(pos, q, k, v, kc, vc)


WO_ROWS = 640
D_FIRST = 768
D_REST = FFN_SHARD - D_FIRST
PIECE = 640
BAND = 16
N_BAND = ROWS // BAND


def combine(a_o, a_st, b_o, b_st):
    lane = lax.broadcasted_iota(jnp.int32, (ROWS, HD), 1)
    is_max = lane < 64
    top = jnp.maximum(a_st, b_st)
    fa = jnp.exp(jnp.where(is_max, a_st - top, 0.0))
    fb = jnp.exp(jnp.where(is_max, b_st - top, 0.0))
    total = pltpu.roll(fa, 64, 1) * a_st + pltpu.roll(fb, 64, 1) * b_st
    out = [fa[:, j:j + 1] * a_o[j] + fb[:, j:j + 1] * b_o[j] for j in range(5)]
    return out, jnp.where(is_max, top, total)


def mlp_kernel(op_ref, x, gain, wo, wg, wu, wd, out_ref,
               wo_buf, g_buf, u_buf, d_buf, rs1, z, rs2, attn_buf,
               stage_p, r1, stage_h, r2, full1, n_buf, a_buf, x_ref, gain_ref,
               sem_w, rs_s, rs_r, p_s, p_r, h_s, h_r, f_s, f_r, g_s, g_r,
               p_s2, p_r2, h_s2, h_r2, f_s2, f_r2, g_s2, g_r2):
    s = lax.axis_index("sp")
    t = lax.axis_index("tp")
    c = lax.rem(s, 2)
    xc = s // 2
    ot, ox, oc = 1 - t, 1 - xc, 1 - c
    core_dev = {"tp": t, "sp": 2 * xc + oc}
    chips = [(t, xc), (t, ox), (ot, xc), (ot, ox)]
    devs = [{"tp": ct, "sp": 2 * cx + c} for ct, cx in chips]
    chip_id = [2 * ct + cx for ct, cx in chips]

    all_here = greet([core_dev] + devs[1:])
    wo_row = pl.multiple_of(s * WO_ROWS, WO_ROWS)
    start = pl.multiple_of(jnp.minimum(s * FFN_SHARD, FFN_LOC - FFN_SHARD), 256)
    half = DIM // 2
    held = pl.ds(start, HELD)
    last = pl.ds(start + HELD, FFN_SHARD - HELD)

    wo_cp = pltpu.make_async_copy(wo.at[pl.ds(wo_row, WO_ROWS), :], wo_buf.at[pl.ds(0, WO_ROWS), :], sem_w.at[0])
    g_cps = [pltpu.make_async_copy(wg.at[pl.ds(i * half, half), held], g_buf.at[pl.ds(i * half, half), :],
                                   sem_w.at[1 + i]) for i in range(2)]
    u_cps = [pltpu.make_async_copy(wu.at[pl.ds(i * half, half), held], u_buf.at[pl.ds(i * half, half), :],
                                   sem_w.at[3 + i]) for i in range(2)]
    d_cp = pltpu.make_async_copy(wd.at[pl.ds(start + D_FIRST, D_REST), :], d_buf, sem_w.at[5])
    d0_cp = pltpu.make_async_copy(wd.at[pl.ds(start, D_FIRST), :], wo_buf, sem_w.at[6])
    own_piece = pl.ds(pl.multiple_of((c * 4 + chip_id[0]) * PIECE, PIECE), PIECE)
    x_cp = pltpu.make_async_copy(x.at[:, own_piece], x_ref, sem_w.at[7])
    gain_cp = pltpu.make_async_copy(gain, gain_ref, sem_w.at[8])
    for cp in (x_cp, gain_cp, wo_cp, g_cps[0]):
        cp.start()
    all_here()

    first = remote(op_ref.at[pl.ds(oc * 2, 2)], rs1, rs_s.at[0], rs_r.at[0], core_dev)
    first.start()
    first.wait_recv()

    def merge(i):
        mine = 2 * c + i
        return combine([op_ref[mine, j] for j in range(5)], op_ref[mine, 5],
                       [rs1[i, j] for j in range(5)], rs1[i, 5])

    o_out, st_out = merge(ox)
    for j in range(5):
        z[j] = o_out[j]
    z[5] = st_out
    second = remote(z, rs2, rs_s.at[1], rs_r.at[1], devs[1])
    second.start()
    o_own, st_own = merge(xc)
    for cp in (x_cp, gain_cp, wo_cp):
        cp.wait()
    for cp in (g_cps[1], u_cps[0], u_cps[1]):
        cp.start()
    second.wait_recv()
    o_all, st_all = combine(o_own, st_own, [rs2[j] for j in range(5)], rs2[5])
    for j in range(5):
        attn_buf[:, j * HD:(j + 1) * HD] = (o_all[j] / st_all[:, 64 + j:65 + j]).astype(BF16)

    def all_reduce(compute, finish, after, stage_p, r1, stage_h, r2, full, p_s, p_r, h_s, h_r, f_s, f_r, g_s, g_r):
        order = (3, 2, 1, 0)
        bands = [pl.ds(i * BAND, BAND) for i in range(N_BAND)]
        to_core = {}
        own, to_chip = None, {}

        def for_core(d):
            stage_p[d] = compute(oc * 4 + chip_id[d])
            to_core[d] = remote(stage_p.at[d], r1.at[d], p_s.at[d], p_r.at[d], core_dev)
            to_core[d].start()

        for_core(order[0])
        for_core(order[1])
        for n, d in enumerate(order):
            part = compute(c * 4 + chip_id[d])
            to_core[d].wait_recv()
            part = part + r1[d]
            if d:
                stage_h[d - 1] = part
                for i, band in enumerate(bands):
                    to_chip[d, i] = remote(stage_h.at[d - 1, band], r2.at[d - 1, band], h_s.at[d - 1, i],
                                           h_r.at[d - 1, i], devs[d])
                    to_chip[d, i].start()
            else:
                own = part
            if n + 2 < 4:
                for_core(order[n + 2])
        after()
        mine = c * 4 + chip_id[0]
        sends, forward = {}, {}
        for i, band in enumerate(bands):
            total = own[i * BAND:(i + 1) * BAND]
            for d in (1, 2, 3):
                to_chip[d, i].wait_recv()
                total = total + r2[d - 1, band]
            full[mine, band] = finish(total, mine, band)
            here = full.at[mine, band]
            for d in (3, 2, 1):
                sends[d, i] = remote(here, here, f_s.at[d - 1, i], f_r.at[d - 1, i], devs[d])
                sends[d, i].start()
            forward[0, i] = remote(here, here, g_s.at[0, i], g_r.at[0, i], core_dev)
            forward[0, i].start()
        for i, band in enumerate(bands):
            for d in (1, 2, 3):
                sends[d, i].wait_recv()
                piece = full.at[c * 4 + chip_id[d], band]
                forward[d, i] = remote(piece, piece, g_s.at[d, i], g_r.at[d, i], core_dev)
                forward[d, i].start()
        for cp in forward.values():
            cp.wait_recv()
        for group in (forward, sends, to_chip, to_core):
            for cp in group.values():
                cp.wait_send()

    def piece_cols(i):
        return pl.ds(pl.multiple_of(i * PIECE, PIECE), PIECE)

    d_cp.start()
    x_f32 = x_ref[...].astype(F32)
    all_reduce(lambda i: jnp.dot(attn_buf[...], wo_buf[:WO_ROWS, piece_cols(i)], preferred_element_type=F32),
               lambda v, i, band: v + x_f32[band.start:band.start + BAND], d0_cp.start,
               stage_p, r1, stage_h, r2, full1, p_s, p_r, h_s, h_r, f_s, f_r, g_s, g_r)
    first.wait_send()
    second.wait_send()

    sq = jnp.zeros((ROWS, 1), F32)
    for i in range(8):
        sq += jnp.sum(jnp.square(full1[i]), axis=-1, keepdims=True)
    inv = lax.rsqrt(sq / DIM + 1e-5)
    blocks = PIECE // HD
    scaled_norm(lambda i: full1[i // blocks, :, (i % blocks) * HD:(i % blocks + 1) * HD], inv, gain_ref, n_buf)

    for cp in g_cps + u_cps:
        cp.wait()
    skip = s * FFN_SHARD - start

    def hidden(j, shift, width):
        at = pl.ds(pl.multiple_of(j * width, 256), width)
        to = pl.ds(pl.multiple_of(j * width + shift, 256), width)
        gate = jnp.dot(n_buf[...], g_buf[:, at], preferred_element_type=F32)
        up = jnp.dot(n_buf[...], u_buf[:, at], preferred_element_type=F32)
        act = gate / (1.0 + jnp.exp(-gate)) * up
        col = lax.broadcasted_iota(jnp.int32, (ROWS, width), 1) + (j * width + shift)
        a_buf[:, to] = jnp.where(col >= skip, act, 0.0).astype(BF16)
        return 0

    tail_cps = [pltpu.make_async_copy(src.at[:, last], buf.at[:, pl.ds(0, 256)], sem_w.at[9 + i])
                for i, (src, buf) in enumerate(((wg, g_buf), (wu, u_buf)))]
    hidden(0, 0, 768)
    for cp in tail_cps:
        cp.start()
    hidden(1, 0, 768)
    for cp in tail_cps:
        cp.wait()
    hidden(0, HELD, 256)

    d_cp.wait()
    d0_cp.wait()

    def down(i):
        at = piece_cols(i)
        return (jnp.dot(a_buf[:, :D_FIRST], wo_buf[:, at], preferred_element_type=F32)
                + jnp.dot(a_buf[:, D_FIRST:], d_buf[:, at], preferred_element_type=F32))

    all_reduce(down, lambda v, i, band: v + full1[i, band], lambda: None,
               stage_p, r1, stage_h, r2, full1, p_s2, p_r2, h_s2, h_r2, f_s2, f_r2, g_s2, g_r2)
    for i in range(8):
        out_ref[:, i * PIECE:(i + 1) * PIECE] = full1[i].astype(BF16)


def mlp_call(op, x, gain, wo, wg, wu, wd):
    dma = pltpu.SemaphoreType.DMA

    def pieces(n):
        return pltpu.VMEM((n, ROWS, PIECE), F32)

    ar_bufs = [pieces(4), pieces(4), pieces(3), pieces(3), pieces(8)]
    ar_sems = [dma((4,)), dma((4,))] + [dma((3, N_BAND))] * 4 + [dma((4, N_BAND))] * 2
    return pl.pallas_call(
        mlp_kernel,
        out_shape=jax.ShapeDtypeStruct((ROWS, DIM), BF16),
        in_specs=[vmem()] + [hbm()] * 6,
        out_specs=vmem(),
        scratch_shapes=[
            pltpu.VMEM((D_FIRST, DIM), BF16), pltpu.VMEM((DIM, HELD), BF16),
            pltpu.VMEM((DIM, HELD), BF16), pltpu.VMEM((D_REST, DIM), BF16),
            pltpu.VMEM((2, 6, ROWS, HD), F32), pltpu.VMEM((6, ROWS, HD), F32), pltpu.VMEM((6, ROWS, HD), F32),
            pltpu.VMEM((ROWS, WO_ROWS), BF16),
        ] + ar_bufs + [
            pltpu.VMEM((ROWS, DIM), BF16), pltpu.VMEM((ROWS, FFN_SHARD), BF16),
            pltpu.VMEM((ROWS, PIECE), BF16), pltpu.VMEM((DIM // HD, HD), BF16), dma((11,)), dma((2,)), dma((2,)),
        ] + ar_sems + ar_sems,
        compiler_params=pltpu.CompilerParams(collective_id=1, has_side_effects=True, vmem_limit_bytes=52 << 20),
        name="mlp",
    )(op, x, gain, wo, wg, wu, wd)


def solution(mesh):
    half_idx = np.arange(HD // 2, dtype=np.float64)
    freq = np.repeat(1.0 / (ROPE_THETA ** (2.0 * half_idx / HD)), 2).astype(np.float32)[None, :]

    def local_step(layer_in, new_pos, k_blk, v_blk, attn_gain, w_query, w_key, w_value, w_out, mlp_gain, w_gate, w_up, w_down):
        kc = jnp.transpose(k_blk, (0, 2, 1, 3))
        vc = jnp.transpose(v_blk, (0, 2, 1, 3))
        hb = lambda a: pltpu.with_memory_space_constraint(a, pltpu.HBM)
        q, k, v, kc = qkv_call(hb(new_pos), hb(layer_in), hb(attn_gain.reshape(DIM // HD, HD)), hb(jnp.asarray(freq)),
                               w_query, w_key, w_value, kc)
        ko, vo, kn, vn, op, _ = attn_call(new_pos, q, k, v, kc, vc)
        out = mlp_call(op, hb(layer_in), hb(mlp_gain.reshape(DIM // HD, HD)), w_out, w_gate, w_up, w_down)
        back = lambda a: jnp.transpose(a, (0, 2, 1, 3))
        return out, back(ko), back(vo), jnp.transpose(kn, (1, 0, 2)), jnp.transpose(vn, (1, 0, 2))

    cache_spec = P('dp', 'sp', 'tp', None)
    new_spec = P('dp', 'tp', None)
    in_specs = (P('dp', None), P('dp'), cache_spec, cache_spec, P(None), P(None, 'tp'), P(None, 'tp'), P(None, 'tp'), P('tp', None), P(None), P(None, 'tp'), P(None, 'tp'), P('tp', None))
    out_specs = (P('dp', None), cache_spec, cache_spec, new_spec, new_spec)
    return jax.shard_map(local_step, mesh=mesh, in_specs=in_specs, out_specs=out_specs, check_vma=False)
```
